128 devices in a mesh: section: 4 (over y), mp: 32 (over x, z, core).
Axes of the slice: x: 4, y: 4, z: 4, core: 2. Of those that a mesh axis runs over, the one named last changes fastest.
Arguments:
- hidden_in: bfloat16 [1, 4, 64, 4096], P(None, 'section'), may hold values from -36 to 36
- attn_gain: bfloat16 [4, 4096], P('section'), may hold values from 0.5 to 2
- w_query: bfloat16 [4, 4096, 4096], P('section', None, 'mp'), may hold values from -0.75 to 0.75
- w_key: bfloat16 [4, 4096, 1024], P('section', None, 'mp'), may hold values from -0.0625 to 0.0625
- w_value: bfloat16 [4, 4096, 1024], P('section', None, 'mp'), may hold values from -0.09375 to 0.09375
- w_out: bfloat16 [4, 4096, 4096], P('section', 'mp'), may hold values from -0.09375 to 0.09375
- ffn_gain: bfloat16 [4, 4096], P('section'), may hold values from 0.5 to 2
- w_gate: bfloat16 [4, 4096, 16384], P('section', None, 'mp'), may hold values from -0.09375 to 0.09375
- w_up: bfloat16 [4, 4096, 16384], P('section', None, 'mp'), may hold values from -0.09375 to 0.09375
- w_down: bfloat16 [4, 16384, 4096], P('section', 'mp'), may hold values from -0.046875 to 0.046875
- ffn_blocks: int32 [4, 4], P(None, 'section'), may hold values from 1 to 112
- heads_on: int32 [4, 4], P(None, 'section'), may hold values from 1 to 32
Outputs:
- hidden_out: bfloat16 [1, 4, 64, 4096], P(None, 'section')
The draws below stay inside these ranges and needn't reach their ends.
Inputs may be any that keep to these rules, and one draw needn't show every extreme that they name: `ffn_blocks`: hidden units below 128 times the entry are active. `heads_on`: query heads below the entry are active.
All inputs are finite; a program needn't handle non-finite values.
Results may differ from the reference program's by a relative error of at most 0.025.
Values may be sent and summed in bfloat16 or wider, within the bound.
A program may use at most 128 MiB of HBM per device.

```python
import math
import jax
import jax.numpy as jnp
from jax import lax

D = 4096
HEADS = 32
KV_HEADS = 8
HD = 128
BLOCK = 128
FFB = 112
FF = 14336
FFP = 16384
SECTIONS = 4
LAYERS = 4
LEN = 64
MICRO_DEV = 1
MICRO = 4
N_MP = 32


def query_key_pair(key):
    folded = jax.random.fold_in(key, 7101)
    key_keys, key_query = jax.random.split(folded, 2)
    query_shape = (LAYERS, D, HEADS * HD)
    key_shape = (LAYERS, D, KV_HEADS * HD)
    spread_scale = D ** (-0.5)
    key_weight = jnp.clip(jax.random.normal(key_keys, key_shape, jnp.float32), -4.0, 4.0) * spread_scale
    query_weight = jnp.clip(jax.random.normal(key_query, query_shape, jnp.float32), -4.0, 4.0) * spread_scale
    return (query_weight, key_weight)


def draw_w_query(key, part):
    return query_key_pair(key)[0].astype(jnp.bfloat16)


def draw_w_key(key, part):
    return query_key_pair(key)[1].astype(jnp.bfloat16)


def draw_hidden_in(key, part):
    folded = jax.random.fold_in(key, 7202)
    key_noise, key_rows, key_columns = jax.random.split(folded, 3)
    array_shape = (MICRO_DEV, SECTIONS, LEN, D)
    low_end = jnp.log(0.3)
    high_end = jnp.log(3.0)
    row_scale = jnp.exp(jax.random.uniform(key_rows, (MICRO_DEV, SECTIONS, LEN, 1), jnp.float32, low_end, high_end))
    col_scale = jnp.exp(jax.random.uniform(key_columns, (1, 1, 1, D), jnp.float32, low_end, high_end))
    jitter = jnp.clip(jax.random.normal(key_noise, array_shape, jnp.float32), -4.0, 4.0)
    return (jitter * row_scale * col_scale).astype(jnp.bfloat16)


def place_ends(array, stream_key, least, high):
    index_at = [jax.random.randint(jax.random.fold_in(stream_key, axis), (), 0, length) for axis, length in enumerate(array.shape)]
    longest = array.shape.index(max(array.shape))
    next_to = index_at[:longest] + [(index_at[longest] + 1) % array.shape[longest]] + index_at[longest + 1:]
    return array.at[tuple(index_at)].set(least).at[tuple(next_to)].set(high)


def shard_levels(stream_key, shape, pieces, smallest, top_value):
    factor_of = 1.0
    for dim, shards_of in pieces:
        steps = jax.random.uniform(jax.random.fold_in(jax.random.fold_in(stream_key, 6), dim), (shards_of,), jnp.float32, smallest / len(pieces), top_value / len(pieces))
        factor_of = factor_of * jnp.repeat(jnp.exp(steps), shape[dim] // shards_of).reshape((-1,) + (1,) * (len(shape) - 1 - dim))
    return factor_of


def centred(key, extent, width, reach, pieces=(), held_as=jnp.bfloat16):
    factor_of = shard_levels(key, extent, pieces, -0.22, 0.18) if pieces else 1.0
    values = jax.random.normal(key, extent, jnp.float32) * width * factor_of
    return jnp.minimum(jnp.maximum(values, -reach), reach).astype(held_as)


def setup_inputs(seed: int = 0) -> dict:
    keys = jax.random.split(jax.random.key(seed), 13)
    hidden_in = draw_hidden_in(jax.random.fold_in(keys[12], 71), 0)
    attn_gain = jnp.clip(jnp.exp(math.log(2.0) - 1.3862944 * jax.random.uniform(keys[1], (LAYERS, D), jnp.float32) ** shard_levels(keys[1], (LAYERS, D), ((0, 4),), -0.2, 0.2)), 0.5, 2.0).astype(jnp.bfloat16)
    w_query = draw_w_query(jax.random.fold_in(keys[12], 71), 0)
    w_key = draw_w_key(jax.random.fold_in(keys[12], 71), 0)
    w_value = centred(keys[4], (LAYERS, D, KV_HEADS * HD), D ** -0.5, 0.09375, ((0, 4), (2, 32)))
    w_out = centred(keys[5], (LAYERS, HEADS * HD, D), (HEADS * HD) ** -0.5, 0.09375, ((0, 4), (1, 32)))
    ffn_gain = jnp.clip(jnp.exp(math.log(2.0) - 1.3862944 * jax.random.uniform(keys[6], (LAYERS, D), jnp.float32) ** shard_levels(keys[6], (LAYERS, D), ((0, 4),), -0.2, 0.2)), 0.5, 2.0).astype(jnp.bfloat16)
    w_gate = centred(keys[7], (LAYERS, D, FFP), D ** -0.5, 0.09375, ((0, 4), (2, 32)))
    w_up = centred(keys[8], (LAYERS, D, FFP), D ** -0.5, 0.09375, ((0, 4), (2, 32)))
    w_down = centred(keys[9], (LAYERS, FFP, D), FF ** -0.5, 0.046875, ((0, 4), (1, 32)))
    ffn_blocks = place_ends(jax.random.randint(keys[10], (MICRO, LAYERS), 1, FFB + 1), jax.random.fold_in(keys[10], 1), 1, FFB).astype(jnp.int32)
    heads_on = place_ends(jax.random.randint(keys[11], (MICRO, LAYERS), 1, HEADS + 1), jax.random.fold_in(keys[11], 1), 1, HEADS).astype(jnp.int32)
    return {"hidden_in": hidden_in, "attn_gain": attn_gain, "w_query": w_query, "w_key": w_key, "w_value": w_value, "w_out": w_out, "ffn_gain": ffn_gain, "w_gate": w_gate, "w_up": w_up, "w_down": w_down, "ffn_blocks": ffn_blocks, "heads_on": heads_on}


ROPE_BASE = 500000.0
EPSILON = 1e-05

def rms_scale(values, gain_row):
    mean_sq = lax.optimization_barrier(jnp.mean(values * values, axis=-1, keepdims=True))
    return values * lax.rsqrt(mean_sq + EPSILON) * gain_row.astype(jnp.float32)

def rotate(values):
    length = values.shape[0]
    half_dim = values.shape[-1] // 2
    frequency = ROPE_BASE ** (-(jnp.arange(half_dim, dtype=jnp.float32) / half_dim))
    angles = jnp.arange(length, dtype=jnp.float32)[:, None] * frequency[None, :]
    cosine_table = jnp.cos(angles)[:, None, :]
    sine_table = jnp.sin(angles)[:, None, :]
    front_half = values[..., :half_dim].astype(jnp.float32)
    back_half = values[..., half_dim:].astype(jnp.float32)
    return jnp.concatenate([front_half * cosine_table - back_half * sine_table, front_half * sine_table + back_half * cosine_table], axis=-1)

def group_sum(left, right):
    length, inner = left.shape
    group_width = inner // N_MP
    left_groups = left.reshape(length, N_MP, group_width).astype(jnp.float32)
    right_groups = right.reshape(N_MP, group_width, right.shape[1]).astype(jnp.float32)
    partials = jnp.einsum('tgk,gkd->gtd', left_groups, right_groups).astype(jnp.bfloat16)
    return lax.optimization_barrier(jnp.sum(partials.astype(jnp.float32), axis=0))

def layer_step(carried, layer_pos, active, block_count, attn_gain, w_query, w_key, w_value, w_out, ffn_gain, w_gate, w_up, w_down):
    length = carried.shape[0]
    group_size = HEADS // KV_HEADS
    residual = carried.astype(jnp.float32)
    normed = rms_scale(residual, attn_gain[layer_pos]).astype(jnp.bfloat16)
    queries = rotate(jnp.dot(normed, w_query[layer_pos], preferred_element_type=jnp.float32).reshape(length, HEADS, HD)).astype(jnp.bfloat16)
    key_proj = jnp.dot(normed, w_key[layer_pos], preferred_element_type=jnp.float32).astype(jnp.bfloat16).reshape(length, HD, KV_HEADS).transpose(0, 2, 1)
    keys_rot = rotate(key_proj).astype(jnp.bfloat16)
    values = jnp.dot(normed, w_value[layer_pos], preferred_element_type=jnp.float32).astype(jnp.bfloat16).reshape(length, HD, KV_HEADS).transpose(0, 2, 1)
    keys_all = jnp.repeat(keys_rot, group_size, axis=1)
    values_all = jnp.repeat(values, group_size, axis=1)
    scores = jnp.einsum('qhd,khd->hqk', queries.astype(jnp.float32), keys_all.astype(jnp.float32)) * HD ** (-0.5)
    causal = jnp.arange(length)[:, None] >= jnp.arange(length)[None, :]
    scores = jnp.where(causal[None], scores, -jnp.inf)
    probabilities = jax.nn.softmax(scores, axis=-1).astype(jnp.bfloat16)
    context = jnp.einsum('hqk,khd->qhd', probabilities.astype(jnp.float32), values_all.astype(jnp.float32))
    head_ids = jnp.arange(HEADS)
    context = jnp.where((head_ids < active)[None, :, None], context, 0.0).astype(jnp.bfloat16)
    attended = residual + group_sum(context.reshape(length, HEADS * HD), w_out[layer_pos])
    normed_ffn = rms_scale(attended, ffn_gain[layer_pos]).astype(jnp.bfloat16)
    gate_part = jnp.dot(normed_ffn, w_gate[layer_pos][:, :FF], preferred_element_type=jnp.float32)
    up_part = jnp.dot(normed_ffn, w_up[layer_pos][:, :FF], preferred_element_type=jnp.float32)
    unit_ids = jnp.arange(FF)
    hidden = jnp.where((unit_ids < BLOCK * block_count)[None, :], jax.nn.silu(gate_part) * up_part, 0.0).astype(jnp.bfloat16)
    padded = jnp.pad(hidden, ((0, 0), (0, w_gate.shape[2] - FF)))
    return (attended + group_sum(padded, w_down[layer_pos])).astype(jnp.bfloat16)

def reference(hidden_in, attn_gain, w_query, w_key, w_value, w_out, ffn_gain, w_gate, w_up, w_down, ffn_blocks, heads_on):
    finished = []
    for micro_index in range(MICRO):
        carried = hidden_in[micro_index // SECTIONS, micro_index % SECTIONS]
        for layer_pos in range(LAYERS):
            carried = layer_step(carried, layer_pos, heads_on[micro_index, layer_pos], ffn_blocks[micro_index, layer_pos], attn_gain, w_query, w_key, w_value, w_out, ffn_gain, w_gate, w_up, w_down)
        finished.append(carried)
    return jnp.stack(finished).reshape(MICRO_DEV, SECTIONS, LEN, D)
```

```python
import functools

import jax
import jax.numpy as jnp
import numpy as np
from jax import lax
from jax.experimental import pallas as pl
from jax.experimental.pallas import tpu as pltpu
from jax.sharding import PartitionSpec as P

HEADS = 32
KV_HEADS = 8
HD = 128
BLOCK = 128
D = 4096
LEN = 64
N = 32
UNITS = 512
MICRO = 4
SECTIONS = 4
ROPE_BASE = 500000.0
EPSILON = 1e-05
MESH = pl.DeviceIdType.MESH
BF = jnp.bfloat16
F32 = jnp.float32
S_AG1, S_KV, S_RS1, S_AG2, S_RS2 = range(5)


def body(
    hid, again, wq, wk, wv, wo, fgain, wg, wu, wd, blocks, heads,
    cs, sn, cst, snt, pk, pv,
    out,
    x0, xa, xb, r1, r2, p1, p2, kvs, kvr, obuf, yb, att, xg, hbuf, qs,
    wqkv, wkb, wvb, wob, wgb, wub, wdb,
    send_sem, recv_sem, xin_sem, yh_sem, misc_sem, w_sem,
):
    sec = lax.axis_index("section")
    me = lax.axis_index("mp")
    head_id = me
    kv_id = me // (HEADS // KV_HEADS)

    def dev(s, d):
        return (s, d)

    def others(fn):
        def step(k, carry):
            fn(lax.rem(me + k, N))
            return carry

        lax.fori_loop(1, N, step, 0)

    loads = [
        (wq.at[0], wqkv.at[:, pl.ds(0, HD)]),
        (wk.at[0], wkb),
        (wv.at[0], wvb),
        (wo.at[0], wob),
        (wg.at[0], wgb),
        (wu.at[0], wub),
        (wd.at[0], wdb),
    ]
    weight = [pltpu.make_async_copy(s, d, w_sem.at[i]) for i, (s, d) in enumerate(loads)]

    def load_hidden(dst, sem):
        def step(j, carry):
            cols = pl.ds(pl.multiple_of(j * 128, 128), 128)
            pltpu.make_async_copy(hid.at[0, 0, :, cols], dst.at[j], sem).start()
            return carry

        lax.fori_loop(0, N, step, 0)

    @pl.when(sec == 0)
    def _():
        load_hidden(xa.at[0], xin_sem.at[0])

    @pl.when(sec != 0)
    def _():
        load_hidden(x0, misc_sem.at[0])

    for w in weight:
        w.start()

    barrier = pltpu.get_barrier_semaphore()

    def greet(d):
        pl.semaphore_signal(barrier, inc=1, device_id=dev(sec, d), device_id_type=MESH)

    others(greet)
    for k in range(1, SECTIONS):
        pl.semaphore_signal(
            barrier, inc=1, device_id=dev(lax.rem(sec + k, SECTIONS), me), device_id_type=MESH
        )

    weight[1].wait()
    weight[2].wait()

    def permute_rows(i, carry):
        rows = pl.ds(pl.multiple_of(i * 512, 512), 512)
        both = jnp.dot(wkb[rows, :], pk[...], preferred_element_type=F32) + jnp.dot(
            wvb[rows, :], pv[...], preferred_element_type=F32
        )
        wqkv[rows, pl.ds(HD, HD)] = both.astype(BF)
        return carry

    lax.fori_loop(0, D // 512, permute_rows, 0)

    pl.semaphore_wait(barrier, N - 1 + SECTIONS - 1)

    @pl.when(sec != 0)
    def _():
        pltpu.make_async_copy(x0, x0, misc_sem.at[0]).wait()
        pltpu.make_async_remote_copy(
            src_ref=x0, dst_ref=xa.at[sec], send_sem=misc_sem.at[1], recv_sem=xin_sem.at[sec],
            device_id=dev(0, me), device_id_type=MESH,
        ).start()

    weight[0].wait()

    def broadcast(src, dst, m, phase):
        def send(d):
            pltpu.make_async_remote_copy(
                src_ref=src, dst_ref=dst, send_sem=send_sem.at[phase, m],
                recv_sem=recv_sem.at[phase, m], device_id=dev(sec, d), device_id_type=MESH,
            ).start()

        others(send)

    def wait_recv(buf, phase, m):
        view = buf.at[m, pl.ds(0, N - 1)]
        pltpu.make_async_copy(view, view, recv_sem.at[phase, m]).wait()

    def wait_send(buf, phase, m):
        view = buf.at[m, pl.ds(0, N - 1)]
        pltpu.make_async_copy(view, view, send_sem.at[phase, m]).wait()

    def scaled(buf, m, gain):
        total = jnp.zeros((LEN, 128), F32)
        for j in range(N):
            value = buf[m, j].astype(F32)
            total = total + value * value
            cols = slice(j * 128, (j + 1) * 128)
            xg[:, cols] = (value * gain[:, cols].astype(F32)).astype(BF)
        mean_sq = jnp.sum(total, axis=-1, keepdims=True) * (1.0 / D)
        return lax.rsqrt(mean_sq + EPSILON)

    def total_of(buf, m):
        total = buf[m, 0].astype(F32)
        for j in range(1, N):
            total = total + buf[m, j].astype(F32)
        return total

    def project(m):
        @pl.when(sec == 0)
        def _():
            pltpu.make_async_copy(xa.at[m], xa.at[m], xin_sem.at[m]).wait()

        @pl.when(sec != 0)
        def _():
            pltpu.make_async_copy(yb.at[m], yb.at[m], yh_sem.at[m]).wait()
            broadcast(xa.at[m, me], xa.at[m, me], m, S_AG1)
            wait_recv(xa, S_AG1, m)

        scale = scaled(xa, m, again)
        qkv = jnp.dot(xg[...], wqkv[...], preferred_element_type=F32) * scale
        kv = qkv[:, HD : 2 * HD].astype(BF).astype(F32)
        turned = kv.T
        pairs = jnp.concatenate([turned[0:32, :], turned[32:64, :]], axis=1)
        kvs[m] = pairs.reshape(KV_HEADS, 4, 128)
        kvr[m, me] = kvs[m, kv_id]

        def send(d):
            pltpu.make_async_remote_copy(
                src_ref=kvs.at[m, d // (HEADS // KV_HEADS)], dst_ref=kvr.at[m, me],
                send_sem=send_sem.at[S_KV, m], recv_sem=recv_sem.at[S_KV, m],
                device_id=dev(sec, d), device_id_type=MESH,
            ).start()

        others(send)
        q = qkv[:, :HD]
        half = HD // 2
        swapped = jnp.concatenate([q[:, half:], q[:, :half]], axis=1)
        qs[m] = (q * cs[...] + swapped * sn[...]).astype(BF)

    def attend(m):
        wait_recv(kvr, S_KV, m)
        both = kvr[m].reshape(HD, 128)
        kt = both[:, :LEN]
        vt = both[:, LEN:].astype(BF)
        half = HD // 2
        u, v = kt[:half], kt[half:]
        keys = jnp.concatenate(
            [u * cst[...] - v * snt[...], u * snt[...] + v * cst[...]], axis=0
        ).astype(BF)
        scores = jnp.dot(qs[m], keys, preferred_element_type=F32) * HD ** (-0.5)
        row = lax.broadcasted_iota(jnp.int32, (LEN, LEN), 0)
        col = lax.broadcasted_iota(jnp.int32, (LEN, LEN), 1)
        scores = jnp.where(row >= col, scores, -jnp.inf)
        top = jnp.max(scores, axis=-1, keepdims=True)
        e = jnp.exp(scores - top)
        prob = (e / jnp.sum(e, axis=-1, keepdims=True)).astype(BF)
        context = lax.dot_general(
            prob, vt, (((1,), (1,)), ((), ())), preferred_element_type=F32
        )
        on = jnp.full((LEN, HD), heads[m, 0], jnp.int32) > head_id
        context = jnp.where(on, context, 0.0).astype(BF)

        def column(i, carry):
            cols = pl.ds(pl.multiple_of(i * 1024, 1024), 1024)
            term = jnp.dot(context, wob[:, cols], preferred_element_type=F32).astype(BF)
            for j in range(8):
                p1[m, i * 8 + j] = term[:, j * 128 : (j + 1) * 128]
            return carry

        lax.fori_loop(0, 4, column, 0)
        scatter(p1, r1, m, S_RS1)

    def scatter(src, dst, m, phase):
        def send(d):
            pltpu.make_async_remote_copy(
                src_ref=src.at[m, d], dst_ref=dst.at[m, me], send_sem=send_sem.at[phase, m],
                recv_sem=recv_sem.at[phase, m], device_id=dev(sec, d), device_id_type=MESH,
            ).start()

        others(send)
        dst[m, me] = src[m, me]

    def attended(m):
        wait_recv(r1, S_RS1, m)
        value = xa[m, me].astype(F32) + total_of(r1, m)
        att[m] = value
        xb[m, me] = value.astype(BF)
        broadcast(xb.at[m, me], xb.at[m, me], m, S_AG2)

    def feed(m):
        wait_recv(xb, S_AG2, m)
        scale = scaled(xb, m, fgain)
        limit = jnp.full((LEN, 256), blocks[m, 0], jnp.int32) * BLOCK

        def unit(i, carry):
            cols = pl.ds(pl.multiple_of(i * 256, 256), 256)
            gate = jnp.dot(xg[...], wgb[:, cols], preferred_element_type=F32) * scale
            up = jnp.dot(xg[...], wub[:, cols], preferred_element_type=F32) * scale
            ids = me * UNITS + i * 256 + lax.broadcasted_iota(jnp.int32, (LEN, 256), 1)
            value = gate / (1.0 + jnp.exp(-gate)) * up
            hbuf[:, cols] = jnp.where(ids < limit, value, 0.0).astype(BF)
            return carry

        lax.fori_loop(0, 2, unit, 0)

        def column(i, carry):
            cols = pl.ds(pl.multiple_of(i * 1024, 1024), 1024)
            term = jnp.dot(hbuf[...], wdb[:, cols], preferred_element_type=F32).astype(BF)
            for j in range(8):
                p2[m, i * 8 + j] = term[:, j * 128 : (j + 1) * 128]
            return carry

        lax.fori_loop(0, 4, column, 0)
        scatter(p2, r2, m, S_RS2)

    def finish(m):
        wait_recv(r2, S_RS2, m)
        yb[m] = (att[m] + total_of(r2, m)).astype(BF)

        @pl.when(sec < SECTIONS - 1)
        def _():
            pltpu.make_async_remote_copy(
                src_ref=yb.at[m], dst_ref=xa.at[m, me], send_sem=send_sem.at[5, m],
                recv_sem=yh_sem.at[m], device_id=dev(sec + 1, me), device_id_type=MESH,
            ).start()

        @pl.when((sec == SECTIONS - 1) & (m < MICRO - 1))
        def _():
            pltpu.make_async_remote_copy(
                src_ref=yb.at[m], dst_ref=obuf.at[me], send_sem=send_sem.at[5, m],
                recv_sem=misc_sem.at[2], device_id=dev(m, me), device_id_type=MESH,
            ).start()

    def micro(m, carry):
        @pl.when(m == 0)
        def _():
            weight[3].wait()

        project(m)
        attend(m)
        attended(m)

        @pl.when(m == 0)
        def _():
            for w in weight[4:]:
                w.wait()

        feed(m)
        finish(m)
        return carry

    lax.fori_loop(0, MICRO, micro, 0)

    @pl.when(sec == SECTIONS - 1)
    def _():
        obuf[me] = yb[MICRO - 1]

    @pl.when(sec != SECTIONS - 1)
    def _():
        pltpu.make_async_copy(yb.at[0], yb.at[0], misc_sem.at[2]).wait()

    def send_out(d):
        pltpu.make_async_remote_copy(
            src_ref=obuf.at[me], dst_ref=obuf.at[me], send_sem=misc_sem.at[3],
            recv_sem=misc_sem.at[4], device_id=dev(sec, d), device_id_type=MESH,
        ).start()

    others(send_out)
    view = obuf.at[pl.ds(0, N - 1)]
    pltpu.make_async_copy(view, view, misc_sem.at[4]).wait()
    done = pltpu.make_async_copy(obuf, out, misc_sem.at[5])
    done.start()

    def drain(m, carry):
        @pl.when(sec != 0)
        def _():
            wait_send(xa, S_AG1, m)

        wait_send(kvr, S_KV, m)
        wait_send(r1, S_RS1, m)
        wait_send(xb, S_AG2, m)
        wait_send(r2, S_RS2, m)

        @pl.when((sec < SECTIONS - 1) | (m < MICRO - 1))
        def _():
            pltpu.make_async_copy(yb.at[m], yb.at[m], send_sem.at[5, m]).wait()

        return carry

    lax.fori_loop(0, MICRO, drain, 0)

    @pl.when(sec != 0)
    def _():
        pltpu.make_async_copy(x0, x0, misc_sem.at[1]).wait()

    pltpu.make_async_copy(view, view, misc_sem.at[3]).wait()
    done.wait()


def tables():
    half = HD // 2
    frequency = ROPE_BASE ** (-(np.arange(half, dtype=np.float64) / half))
    angles = np.arange(LEN, dtype=np.float64)[:, None] * frequency[None, :]
    c, s = np.cos(angles).astype(np.float32), np.sin(angles).astype(np.float32)
    cs = np.concatenate([c, c], axis=1)
    sn = np.concatenate([-s, s], axis=1)
    pk = np.zeros((32, HD), np.float32)
    pv = np.zeros((32, HD), np.float32)
    for j in range(4):
        for k in range(KV_HEADS):
            pk[j * KV_HEADS + k, k * 4 + j] = 1.0
            pv[j * KV_HEADS + k, 32 + k * 4 + j] = 1.0
    return (
        jnp.asarray(cs), jnp.asarray(sn),
        jnp.asarray(np.ascontiguousarray(c.T)), jnp.asarray(np.ascontiguousarray(s.T)),
        jnp.asarray(pk, BF), jnp.asarray(pv, BF),
    )


def per_device(*args):
    any_spec = pl.BlockSpec(memory_space=pl.ANY)
    vmem = pl.BlockSpec(memory_space=pltpu.VMEM)
    smem = pl.BlockSpec(memory_space=pltpu.SMEM)
    piece = (LEN, 128)
    whole = (MICRO, N, *piece)
    gathered = pl.pallas_call(
        body,
        out_shape=jax.ShapeDtypeStruct((N, *piece), BF),
        in_specs=[
            any_spec, vmem, any_spec, any_spec, any_spec, any_spec, vmem, any_spec, any_spec,
            any_spec, smem, smem, vmem, vmem, vmem, vmem, vmem, vmem,
        ],
        out_specs=any_spec,
        scratch_shapes=[
            pltpu.VMEM((N, *piece), BF),
            pltpu.VMEM(whole, BF),
            pltpu.VMEM(whole, BF),
            pltpu.VMEM(whole, BF),
            pltpu.VMEM(whole, BF),
            pltpu.VMEM(whole, BF),
            pltpu.VMEM(whole, BF),
            pltpu.VMEM((MICRO, KV_HEADS, 4, 128), F32),
            pltpu.VMEM((MICRO, N, 4, 128), F32),
            pltpu.VMEM((N, *piece), BF),
            pltpu.VMEM((MICRO, *piece), BF),
            pltpu.VMEM((MICRO, *piece), F32),
            pltpu.VMEM((LEN, D), BF),
            pltpu.VMEM((LEN, UNITS), BF),
            pltpu.VMEM((MICRO, *piece), BF),
            pltpu.VMEM((D, 256), BF),
            pltpu.VMEM((D, 32), BF),
            pltpu.VMEM((D, 32), BF),
            pltpu.VMEM((HD, D), BF),
            pltpu.VMEM((D, UNITS), BF),
            pltpu.VMEM((D, UNITS), BF),
            pltpu.VMEM((UNITS, D), BF),
            pltpu.SemaphoreType.DMA((6, MICRO)),
            pltpu.SemaphoreType.DMA((5, MICRO)),
            pltpu.SemaphoreType.DMA((MICRO,)),
            pltpu.SemaphoreType.DMA((MICRO,)),
            pltpu.SemaphoreType.DMA((6,)),
            pltpu.SemaphoreType.DMA((7,)),
        ],
        compiler_params=pltpu.CompilerParams(
            collective_id=0, has_side_effects=True, vmem_limit_bytes=56 * 1024 * 1024
        ),
    )(*args, *tables())
    return gathered.transpose(1, 0, 2).reshape(1, 1, LEN, D)


def solution(mesh):
    return jax.shard_map(
        per_device,
        mesh=mesh,
        in_specs=(
            P(None, "section", None, None),
            P("section", None),
            P("section", None, "mp"),
            P("section", None, "mp"),
            P("section", None, "mp"),
            P("section", "mp", None),
            P("section", None),
            P("section", None, "mp"),
            P("section", None, "mp"),
            P("section", "mp", None),
            P(None, "section"),
            P(None, "section"),
        ),
        out_specs=P(None, "section", None, None),
        check_vma=False,
    )
```

```python
import functools

import jax
import jax.numpy as jnp
import numpy as np
from jax import lax
from jax.experimental import pallas as pl
from jax.experimental.pallas import tpu as pltpu
from jax.sharding import PartitionSpec as P

HEADS = 32
KV_HEADS = 8
HD = 128
BLOCK = 128
D = 4096
LEN = 64
N = 32
UNITS = 512
MICRO = 4
SECTIONS = 4
ROPE_BASE = 500000.0
EPSILON = 1e-05
MESH = pl.DeviceIdType.MESH
BF = jnp.bfloat16
F32 = jnp.float32
CHIPS = 16
(
    S_IN, S_Y, S_AG1, S_PASS1, S_KV, S_GIVE1, S_RS1, S_RS2, S_AG2, S_PASS2, S_GIVE2, S_AG3, S_PASS3,
) = range(13)
RING = (0, 1, 2, 1)
FAR_FIRST = sorted(
    [(dx, dz) for dx in range(4) for dz in range(4) if (dx, dz) != (0, 0)],
    key=lambda d: -(RING[d[0]] + RING[d[1]]),
)


def body(
    hid, again, wq, wk, wv, wo, fgain, wg, wu, wd, blocks, heads,
    cs, sn, cst, snt, pk, pv,
    out,
    x0, xa, xb, r1, r2, pt, ps, dr, own, kvs, kvr, obuf, yb, att, xg, acc, hbuf, qs,
    wqkv, wkb, wvb, wob, wgb, wub, wdb,
    send_sem, recv_sem, misc_sem, w_sem,
):
    sec = lax.axis_index("section")
    me = lax.axis_index("mp")
    chip = me // 2
    core = lax.rem(me, 2)
    rest = 1 - core
    partner = chip * 2 + rest
    mine = core * CHIPS + chip
    kv_id = me // (HEADS // KV_HEADS)
    at_x, at_z = chip // 4, lax.rem(chip, 4)

    def others(fn):
        for dx, dz in FAR_FIRST:
            fn(lax.rem(at_x + dx, 4) * 4 + lax.rem(at_z + dz, 4))

    def remote(src, dst, phase, m, s, d):
        return pltpu.make_async_remote_copy(
            src_ref=src, dst_ref=dst, send_sem=send_sem.at[phase, m],
            recv_sem=recv_sem.at[phase, m], device_id=(s, d), device_id_type=MESH,
        )

    def received(view, phase, m):
        pltpu.make_async_copy(view, view, recv_sem.at[phase, m]).wait()

    def sent(view, phase, m):
        pltpu.make_async_copy(view, view, send_sem.at[phase, m]).wait()

    def half(which):
        return pl.ds(pl.multiple_of(which * CHIPS, CHIPS), CHIPS)

    loads = [
        (wk.at[0], wkb),
        (wv.at[0], wvb),
        (wq.at[0], wqkv.at[:, pl.ds(0, HD)]),
        (wo.at[0], wob),
        (wg.at[0], wgb),
        (wu.at[0], wub),
        (wd.at[0], wdb),
    ]
    weight = [pltpu.make_async_copy(s, d, w_sem.at[i]) for i, (s, d) in enumerate(loads)]

    def load_hidden(dst, first, sem):
        def step(j, carry):
            cols = pl.ds(pl.multiple_of((core * CHIPS + j) * 128, 128), 128)
            pltpu.make_async_copy(hid.at[0, 0, :, cols], dst.at[first + j], sem).start()
            return carry

        lax.fori_loop(0, CHIPS, step, 0)

    @pl.when(sec == 0)
    def _():
        load_hidden(xa.at[0], core * CHIPS, recv_sem.at[S_IN, 0])

    @pl.when(sec != 0)
    def _():
        load_hidden(x0, 0, misc_sem.at[0])

    for w in weight:
        w.start()

    barrier = pltpu.get_barrier_semaphore()

    def greet(k, carry):
        pl.semaphore_signal(
            barrier, inc=1, device_id=(sec, lax.rem(me + k, N)), device_id_type=MESH
        )
        return carry

    lax.fori_loop(1, N, greet, 0)
    for k in range(1, SECTIONS):
        pl.semaphore_signal(
            barrier, inc=1, device_id=(lax.rem(sec + k, SECTIONS), me), device_id_type=MESH
        )

    weight[0].wait()
    weight[1].wait()

    def permute_rows(i, carry):
        rows = pl.ds(pl.multiple_of(i * 512, 512), 512)
        both = jnp.dot(wkb[rows, :], pk[...], preferred_element_type=F32) + jnp.dot(
            wvb[rows, :], pv[...], preferred_element_type=F32
        )
        wqkv[rows, pl.ds(HD, HD)] = both.astype(BF)
        return carry

    lax.fori_loop(0, D // 512, permute_rows, 0)

    pl.semaphore_wait(barrier, N - 1 + SECTIONS - 1)

    @pl.when(sec != 0)
    def _():
        pltpu.make_async_copy(x0, x0, misc_sem.at[0]).wait()
        pltpu.make_async_remote_copy(
            src_ref=x0, dst_ref=xa.at[sec, half(core)], send_sem=misc_sem.at[1],
            recv_sem=recv_sem.at[S_IN, sec], device_id=(0, me), device_id_type=MESH,
        ).start()

    weight[2].wait()

    def gather_send(buf, phase, m):
        view = buf.at[m, mine]
        others(lambda chip_to: remote(view, view, phase, m, sec, chip_to * 2 + core).start())

    def gather_pass(buf, phase, m):
        view = buf.at[m, half(core)]
        remote(view, view, phase, m, sec, partner).start()

    def scaled(buf, m, which, slot, gain):
        total = jnp.zeros((LEN, 128), F32)
        for j in range(CHIPS):
            block = which * CHIPS + j
            value = buf[m, block].astype(F32)
            total = total + value * value
            factor = gain[:, pl.ds(pl.multiple_of(block * 128, 128), 128)].astype(F32)
            xg[slot, :, j * 128 : (j + 1) * 128] = (value * factor).astype(BF)
        return total

    def inverse_rms(total):
        mean_sq = jnp.sum(total, axis=-1, keepdims=True) * (1.0 / D)
        return lax.rsqrt(mean_sq + EPSILON)

    def rows_of(which):
        return pl.ds(pl.multiple_of(which * (D // 2), D // 2), D // 2)

    def arrive(m):
        @pl.when(sec != 0)
        def _():
            received(yb.at[m], S_Y, m)
            gather_send(xa, S_AG1, m)

    def project(m):
        @pl.when(sec == 0)
        def _():
            received(xa.at[m, pl.ds(0, CHIPS)], S_IN, m)

        @pl.when(sec != 0)
        def _():
            received(xa.at[m, pl.ds(0, CHIPS - 1)], S_AG1, m)

        gather_pass(xa, S_PASS1, m)
        total = scaled(xa, m, core, 0, again)
        qkv = jnp.dot(xg[0], wqkv[rows_of(core), :], preferred_element_type=F32)
        received(xa.at[m, pl.ds(0, CHIPS)], S_PASS1, m)
        total = total + scaled(xa, m, rest, 1, again)
        qkv = qkv + jnp.dot(xg[1], wqkv[rows_of(rest), :], preferred_element_type=F32)
        qkv = qkv * inverse_rms(total)
        kv = qkv[:, HD : 2 * HD].astype(BF).astype(F32)
        turned = kv.T
        pairs = jnp.concatenate([turned[0:32, :], turned[32:64, :]], axis=1)
        kvs[m] = pairs.reshape(KV_HEADS, 4, 128)
        kvr[m, me] = kvs[m, kv_id]

        def send(k, carry):
            d = lax.rem(me + k, N)
            remote(
                kvs.at[m, d // (HEADS // KV_HEADS)], kvr.at[m, me], S_KV, m, sec, d
            ).start()
            return carry

        lax.fori_loop(1, N, send, 0)
        q = qkv[:, :HD]
        mid = HD // 2
        swapped = jnp.concatenate([q[:, mid:], q[:, :mid]], axis=1)
        qs[m] = (q * cs[...] + swapped * sn[...]).astype(BF)

    def reduce_send(left, weights, phase, pass_phase, recv, m):
        def term(which, i):
            first = which * (D // 2) + i * 1024
            cols = pl.ds(pl.multiple_of(first, 1024), 1024)
            return jnp.dot(left, weights[:, cols], preferred_element_type=F32)

        def away(i, carry):
            value = term(rest, i).astype(BF)
            for j in range(8):
                pt[phase - S_RS1, m, i * 8 + j] = value[:, j * 128 : (j + 1) * 128]
            return carry

        lax.fori_loop(0, 2, away, 0)
        give = remote(pt.at[phase - S_RS1, m], dr.at[phase - S_RS1, m], pass_phase, m, sec, partner)
        give.start()

        def kept(i, carry):
            value = term(core, i)
            for j in range(8):
                own[i * 8 + j] = value[:, j * 128 : (j + 1) * 128]
            return carry

        lax.fori_loop(0, 2, kept, 0)
        give.wait()

        def add(j, carry):
            ps[phase - S_RS1, m, j] = (own[j] + dr[phase - S_RS1, m, j].astype(F32)).astype(BF)
            return carry

        lax.fori_loop(0, CHIPS, add, 0, unroll=4)
        others(
            lambda chip_to: remote(
                ps.at[phase - S_RS1, m, chip_to], recv.at[m, chip], phase, m, sec,
                chip_to * 2 + core,
            ).start()
        )
        recv[m, chip] = ps[phase - S_RS1, m, chip]

    def summed(recv, phase, m):
        received(recv.at[m, pl.ds(0, CHIPS - 1)], phase, m)
        total = recv[m, 0].astype(F32)
        for j in range(1, CHIPS):
            total = total + recv[m, j].astype(F32)
        return total

    def attend(m):
        received(kvr.at[m, pl.ds(0, N - 1)], S_KV, m)
        both = kvr[m].reshape(HD, 128)
        kt = both[:, :LEN]
        vt = both[:, LEN:].astype(BF)
        mid = HD // 2
        u, v = kt[:mid], kt[mid:]
        keys = jnp.concatenate(
            [u * cst[...] - v * snt[...], u * snt[...] + v * cst[...]], axis=0
        ).astype(BF)
        scores = jnp.dot(qs[m], keys, preferred_element_type=F32) * HD ** (-0.5)
        row = lax.broadcasted_iota(jnp.int32, (LEN, LEN), 0)
        col = lax.broadcasted_iota(jnp.int32, (LEN, LEN), 1)
        scores = jnp.where(row >= col, scores, -jnp.inf)
        top = jnp.max(scores, axis=-1, keepdims=True)
        e = jnp.exp(scores - top)
        prob = (e / jnp.sum(e, axis=-1, keepdims=True)).astype(BF)
        context = lax.dot_general(
            prob, vt, (((1,), (1,)), ((), ())), preferred_element_type=F32
        )
        on = jnp.full((LEN, HD), heads[m, 0], jnp.int32) > me
        context = jnp.where(on, context, 0.0).astype(BF)
        reduce_send(context, wob, S_RS1, S_GIVE1, r1, m)

    def attended(m):
        value = xa[m, mine].astype(F32) + summed(r1, S_RS1, m)
        att[m] = value
        xb[m, mine] = value.astype(BF)
        gather_send(xb, S_AG2, m)

    def feed(m):
        received(xb.at[m, pl.ds(0, CHIPS - 1)], S_AG2, m)
        gather_pass(xb, S_PASS2, m)
        total = scaled(xb, m, core, 0, fgain)

        def first(i, carry):
            cols = pl.ds(pl.multiple_of(i * 256, 256), 256)
            acc[0, :, cols] = jnp.dot(
                xg[0], wgb[rows_of(core), cols], preferred_element_type=F32
            )
            acc[1, :, cols] = jnp.dot(
                xg[0], wub[rows_of(core), cols], preferred_element_type=F32
            )
            return carry

        lax.fori_loop(0, 2, first, 0)
        received(xb.at[m, pl.ds(0, CHIPS)], S_PASS2, m)
        scale = inverse_rms(total + scaled(xb, m, rest, 1, fgain))
        limit = jnp.full((LEN, 256), blocks[m, 0], jnp.int32) * BLOCK

        def second(i, carry):
            cols = pl.ds(pl.multiple_of(i * 256, 256), 256)
            gate = acc[0, :, cols] + jnp.dot(
                xg[1], wgb[rows_of(rest), cols], preferred_element_type=F32
            )
            up = acc[1, :, cols] + jnp.dot(
                xg[1], wub[rows_of(rest), cols], preferred_element_type=F32
            )
            gate, up = gate * scale, up * scale
            ids = me * UNITS + i * 256 + lax.broadcasted_iota(jnp.int32, (LEN, 256), 1)
            value = gate / (1.0 + jnp.exp(-gate)) * up
            hbuf[:, cols] = jnp.where(ids < limit, value, 0.0).astype(BF)
            return carry

        lax.fori_loop(0, 2, second, 0)
        reduce_send(hbuf[...], wdb, S_RS2, S_GIVE2, r2, m)

    def finish(m):
        yb[m] = (att[m] + summed(r2, S_RS2, m)).astype(BF)

        @pl.when(sec < SECTIONS - 1)
        def _():
            remote(yb.at[m], xa.at[m, mine], S_Y, m, sec + 1, me).start()

        @pl.when((sec == SECTIONS - 1) & (m < MICRO - 1))
        def _():
            pltpu.make_async_remote_copy(
                src_ref=yb.at[m], dst_ref=obuf.at[0, mine], send_sem=send_sem.at[S_Y, m],
                recv_sem=misc_sem.at[2], device_id=(m, me), device_id_type=MESH,
            ).start()

    def slot(i, carry):
        @pl.when(i < MICRO)
        def _():
            arrive(i)
            project(i)

        @pl.when(i == 0)
        def _():
            weight[3].wait()

        @pl.when(i == 1)
        def _():
            for w in weight[4:]:
                w.wait()

        @pl.when(i > 0)
        def _():
            feed(i - 1)

        @pl.when(i < MICRO)
        def _():
            attend(i)

        @pl.when(i > 0)
        def _():
            finish(i - 1)

        @pl.when(i < MICRO)
        def _():
            attended(i)

        return carry

    lax.fori_loop(0, MICRO + 1, slot, 0)

    @pl.when(sec == SECTIONS - 1)
    def _():
        obuf[0, mine] = yb[MICRO - 1]

    @pl.when(sec != SECTIONS - 1)
    def _():
        pltpu.make_async_copy(yb.at[0], yb.at[0], misc_sem.at[2]).wait()

    gather_send(obuf, S_AG3, 0)
    received(obuf.at[0, pl.ds(0, CHIPS - 1)], S_AG3, 0)
    gather_pass(obuf, S_PASS3, 0)
    near = pltpu.make_async_copy(
        obuf.at[0, half(core)], out.at[half(core)], misc_sem.at[3]
    )
    near.start()

    def drain(m, carry):
        @pl.when(sec != 0)
        def _():
            sent(xa.at[m, pl.ds(0, CHIPS - 1)], S_AG1, m)

        sent(xa.at[m, pl.ds(0, CHIPS)], S_PASS1, m)
        sent(kvr.at[m, pl.ds(0, N - 1)], S_KV, m)
        sent(r1.at[m, pl.ds(0, CHIPS - 1)], S_RS1, m)
        sent(xb.at[m, pl.ds(0, CHIPS - 1)], S_AG2, m)
        sent(xb.at[m, pl.ds(0, CHIPS)], S_PASS2, m)
        sent(r2.at[m, pl.ds(0, CHIPS - 1)], S_RS2, m)

        @pl.when((sec < SECTIONS - 1) | (m < MICRO - 1))
        def _():
            sent(yb.at[m], S_Y, m)

        return carry

    lax.fori_loop(0, MICRO, drain, 0)

    @pl.when(sec != 0)
    def _():
        pltpu.make_async_copy(x0, x0, misc_sem.at[1]).wait()

    sent(obuf.at[0, pl.ds(0, CHIPS - 1)], S_AG3, 0)
    received(obuf.at[0, pl.ds(0, CHIPS)], S_PASS3, 0)
    far = pltpu.make_async_copy(obuf.at[0, half(rest)], out.at[half(rest)], misc_sem.at[4])
    far.start()
    sent(obuf.at[0, pl.ds(0, CHIPS)], S_PASS3, 0)
    near.wait()
    far.wait()


def tables():
    half = HD // 2
    frequency = ROPE_BASE ** (-(np.arange(half, dtype=np.float64) / half))
    angles = np.arange(LEN, dtype=np.float64)[:, None] * frequency[None, :]
    c, s = np.cos(angles).astype(np.float32), np.sin(angles).astype(np.float32)
    cs = np.concatenate([c, c], axis=1)
    sn = np.concatenate([-s, s], axis=1)
    pk = np.zeros((32, HD), np.float32)
    pv = np.zeros((32, HD), np.float32)
    for j in range(4):
        for k in range(KV_HEADS):
            pk[j * KV_HEADS + k, k * 4 + j] = 1.0
            pv[j * KV_HEADS + k, 32 + k * 4 + j] = 1.0
    return (
        jnp.asarray(cs), jnp.asarray(sn),
        jnp.asarray(np.ascontiguousarray(c.T)), jnp.asarray(np.ascontiguousarray(s.T)),
        jnp.asarray(pk, BF), jnp.asarray(pv, BF),
    )


def per_device(*args):
    any_spec = pl.BlockSpec(memory_space=pl.ANY)
    vmem = pl.BlockSpec(memory_space=pltpu.VMEM)
    smem = pl.BlockSpec(memory_space=pltpu.SMEM)
    piece = (LEN, 128)
    gathered = pl.pallas_call(
        body,
        out_shape=jax.ShapeDtypeStruct((N, *piece), BF),
        in_specs=[
            any_spec, vmem, any_spec, any_spec, any_spec, any_spec, vmem, any_spec, any_spec,
            any_spec, smem, smem, vmem, vmem, vmem, vmem, vmem, vmem,
        ],
        out_specs=any_spec,
        scratch_shapes=[
            pltpu.VMEM((CHIPS, *piece), BF),
            pltpu.VMEM((MICRO, N, *piece), BF),
            pltpu.VMEM((MICRO, N, *piece), BF),
            pltpu.VMEM((MICRO, CHIPS, *piece), BF),
            pltpu.VMEM((MICRO, CHIPS, *piece), BF),
            pltpu.VMEM((2, MICRO, CHIPS, *piece), BF),
            pltpu.VMEM((2, MICRO, CHIPS, *piece), BF),
            pltpu.VMEM((2, MICRO, CHIPS, *piece), BF),
            pltpu.VMEM((CHIPS, *piece), F32),
            pltpu.VMEM((MICRO, KV_HEADS, 4, 128), F32),
            pltpu.VMEM((MICRO, N, 4, 128), F32),
            pltpu.VMEM((1, N, *piece), BF),
            pltpu.VMEM((MICRO, *piece), BF),
            pltpu.VMEM((MICRO, *piece), F32),
            pltpu.VMEM((2, LEN, D // 2), BF),
            pltpu.VMEM((2, LEN, UNITS), F32),
            pltpu.VMEM((LEN, UNITS), BF),
            pltpu.VMEM((MICRO, *piece), BF),
            pltpu.VMEM((D, 256), BF),
            pltpu.VMEM((D, 32), BF),
            pltpu.VMEM((D, 32), BF),
            pltpu.VMEM((HD, D), BF),
            pltpu.VMEM((D, UNITS), BF),
            pltpu.VMEM((D, UNITS), BF),
            pltpu.VMEM((UNITS, D), BF),
            pltpu.SemaphoreType.DMA((13, MICRO)),
            pltpu.SemaphoreType.DMA((13, MICRO)),
            pltpu.SemaphoreType.DMA((5,)),
            pltpu.SemaphoreType.DMA((7,)),
        ],
        compiler_params=pltpu.CompilerParams(
            collective_id=0, has_side_effects=True, vmem_limit_bytes=56 * 1024 * 1024
        ),
    )(*args, *tables())
    return gathered.transpose(1, 0, 2).reshape(1, 1, LEN, D)


def solution(mesh):
    return jax.shard_map(
        per_device,
        mesh=mesh,
        in_specs=(
            P(None, "section", None, None),
            P("section", None),
            P("section", None, "mp"),
            P("section", None, "mp"),
            P("section", None, "mp"),
            P("section", "mp", None),
            P("section", None),
            P("section", None, "mp"),
            P("section", None, "mp"),
            P("section", "mp", None),
            P(None, "section"),
            P(None, "section"),
        ),
        out_specs=P(None, "section", None, None),
        check_vma=False,
    )
```

```python
import functools

import jax
import jax.numpy as jnp
import numpy as np
from jax import lax
from jax.experimental import pallas as pl
from jax.experimental.pallas import tpu as pltpu
from jax.sharding import PartitionSpec as P

HEADS = 32
KV_HEADS = 8
HD = 128
BLOCK = 128
D = 4096
LEN = 64
N = 32
UNITS = 512
MICRO = 4
SECTIONS = 4
ROPE_BASE = 500000.0
EPSILON = 1e-05
MESH = pl.DeviceIdType.MESH
BF = jnp.bfloat16
F32 = jnp.float32
CHIPS = 16
(
    S_IN, S_Y, S_AG1, S_PASS1, S_KV, S_GIVE1, S_RS1, S_RS2, S_AG2, S_PASS2, S_GIVE2, S_AG3, S_PASS3,
    S_W,
) = range(14)
RING = (0, 1, 2, 1)
FAR_FIRST = sorted(
    [(dx, dz) for dx in range(4) for dz in range(4) if (dx, dz) != (0, 0)],
    key=lambda d: -(RING[d[0]] + RING[d[1]]),
)


def body(
    hid, again, wq, wk, wv, wo, fgain, wg, wu, wd, blocks, heads,
    cs, sn, pk, pv, tk, tv, order,
    out,
    x0, xa, xb, r1, r2, pt, ps, dr, own, kvs, kvr, obuf, yb, att, xg, acc, hbuf, qs,
    ks, vs, aq, wgive, wtake, wqkv, wkb, wvb, wob, wgb, wub, wdb,
    send_sem, recv_sem, misc_sem, w_sem,
):
    sec = lax.axis_index("section")
    me = lax.axis_index("mp")
    chip = me // 2
    core = lax.rem(me, 2)
    rest = 1 - core
    partner = chip * 2 + rest
    mine = core * CHIPS + chip
    kv_id = me // (HEADS // KV_HEADS)
    at_x, at_z = chip // 4, lax.rem(chip, 4)

    def others(fn):
        for dx, dz in FAR_FIRST:
            fn(lax.rem(at_x + dx, 4) * 4 + lax.rem(at_z + dz, 4))

    def remote(src, dst, phase, m, s, d):
        return pltpu.make_async_remote_copy(
            src_ref=src, dst_ref=dst, send_sem=send_sem.at[phase, m],
            recv_sem=recv_sem.at[phase, m], device_id=(s, d), device_id_type=MESH,
        )

    def received(view, phase, m):
        pltpu.make_async_copy(view, view, recv_sem.at[phase, m]).wait()

    def sent(view, phase, m):
        pltpu.make_async_copy(view, view, send_sem.at[phase, m]).wait()

    def half(which):
        return pl.ds(pl.multiple_of(which * CHIPS, CHIPS), CHIPS)

    loads = [
        (wk.at[0], wkb),
        (wv.at[0], wvb),
        (wq.at[0], wqkv.at[:, pl.ds(0, HD)]),
        (wo.at[0], wob),
        (wg.at[0], wgb),
        (wu.at[0], wub),
        (wd.at[0], wdb),
    ]
    weight = [pltpu.make_async_copy(s, d, w_sem.at[i]) for i, (s, d) in enumerate(loads)]

    def load_hidden(dst, first, sem):
        def step(j, carry):
            cols = pl.ds(pl.multiple_of((core * CHIPS + j) * 128, 128), 128)
            pltpu.make_async_copy(hid.at[0, 0, :, cols], dst.at[first + j], sem).start()
            return carry

        lax.fori_loop(0, CHIPS, step, 0)

    @pl.when(sec == 0)
    def _():
        load_hidden(xa.at[0], core * CHIPS, recv_sem.at[S_IN, 0])

    @pl.when(sec != 0)
    def _():
        load_hidden(x0, 0, misc_sem.at[0])

    for w in weight:
        w.start()

    barrier = pltpu.get_barrier_semaphore()

    def greet(k, carry):
        pl.semaphore_signal(
            barrier, inc=1, device_id=(sec, lax.rem(me + k, N)), device_id_type=MESH
        )
        return carry

    lax.fori_loop(1, N, greet, 0)
    for k in range(1, SECTIONS):
        pl.semaphore_signal(
            barrier, inc=1, device_id=(lax.rem(sec + k, SECTIONS), me), device_id_type=MESH
        )

    weight[0].wait()
    weight[1].wait()
    nt = (((1,), (1,)), ((), ()))

    def permute_rows(i, carry):
        rows = pl.ds(pl.multiple_of(i * 512, 512), 512)
        both = jnp.dot(wkb[rows, :], pk[...], preferred_element_type=F32) + jnp.dot(
            wvb[rows, :], pv[...], preferred_element_type=F32
        )
        wqkv[rows, pl.ds(HD, HD)] = both.astype(BF)
        return carry

    def turn_rows(i, carry):
        rows = pl.ds(pl.multiple_of(i * 512, 512), 512)
        both = lax.dot_general(
            tk[...], wkb[rows, :], nt, preferred_element_type=F32
        ) + lax.dot_general(tv[...], wvb[rows, :], nt, preferred_element_type=F32)
        wgive[:, :, rows] = both.reshape(KV_HEADS, 8, 512).astype(BF)
        return carry

    @pl.when(sec == 0)
    def _():
        lax.fori_loop(0, D // 512, permute_rows, 0)

    @pl.when(sec != 0)
    def _():
        lax.fori_loop(0, D // 512, turn_rows, 0)

    pl.semaphore_wait(barrier, N - 1 + SECTIONS - 1)

    @pl.when(sec != 0)
    def _():
        pltpu.make_async_copy(x0, x0, misc_sem.at[0]).wait()
        pltpu.make_async_remote_copy(
            src_ref=x0, dst_ref=xa.at[sec, half(core)], send_sem=misc_sem.at[1],
            recv_sem=recv_sem.at[S_IN, sec], device_id=(0, me), device_id_type=MESH,
        ).start()
        others(
            lambda chip_to: remote(
                wgive.at[chip_to // 2], wtake.at[mine], S_W, 0, sec, chip_to * 2 + core
            ).start()
        )
        wtake[mine] = wgive[chip // 2]
        received(wtake.at[pl.ds(0, CHIPS - 1)], S_W, 0)
        view = wtake.at[half(core)]
        swap = remote(view, view, S_W, 1, sec, partner)
        swap.start()
        swap.wait()

        def put_in_order(i, carry):
            rows = pl.ds(pl.multiple_of(i * 512, 512), 512)
            chunk = wtake[:, :, rows].astype(F32).reshape(2 * HD, 512).T.astype(BF)
            wqkv[rows, pl.ds(HD, 2 * HD)] = jnp.dot(
                chunk, order[...], preferred_element_type=F32
            ).astype(BF)
            return carry

        lax.fori_loop(0, D // 512, put_in_order, 0)
        sent(wtake.at[pl.ds(0, CHIPS - 1)], S_W, 0)

    weight[2].wait()

    def gather_send(buf, phase, m):
        view = buf.at[m, mine]
        others(lambda chip_to: remote(view, view, phase, m, sec, chip_to * 2 + core).start())

    def gather_pass(buf, phase, m):
        view = buf.at[m, half(core)]
        remote(view, view, phase, m, sec, partner).start()

    def scaled(buf, m, which, slot, gain):
        total = jnp.zeros((LEN, 128), F32)
        for j in range(CHIPS):
            block = which * CHIPS + j
            value = buf[m, block].astype(F32)
            total = total + value * value
            factor = gain[:, pl.ds(pl.multiple_of(block * 128, 128), 128)].astype(F32)
            xg[slot, :, j * 128 : (j + 1) * 128] = (value * factor).astype(BF)
        return total

    def inverse_rms(total):
        mean_sq = jnp.sum(total, axis=-1, keepdims=True) * (1.0 / D)
        return lax.rsqrt(mean_sq + EPSILON)

    def rows_of(which):
        return pl.ds(pl.multiple_of(which * (D // 2), D // 2), D // 2)

    def arrive(m):
        @pl.when(sec != 0)
        def _():
            received(yb.at[m], S_Y, m)
            gather_send(xa, S_AG1, m)

    def project(m):
        @pl.when(sec == 0)
        def _():
            received(xa.at[m, pl.ds(0, CHIPS)], S_IN, m)

        @pl.when(sec != 0)
        def _():
            received(xa.at[m, pl.ds(0, CHIPS - 1)], S_AG1, m)

        gather_pass(xa, S_PASS1, m)
        total = scaled(xa, m, core, 0, again)
        front, back = pl.ds(0, 2 * HD), pl.ds(2 * HD, HD)
        aq[:, front] = jnp.dot(xg[0], wqkv[rows_of(core), front], preferred_element_type=F32)

        @pl.when(sec != 0)
        def _():
            aq[:, back] = jnp.dot(xg[0], wqkv[rows_of(core), back], preferred_element_type=F32)

        received(xa.at[m, pl.ds(0, CHIPS)], S_PASS1, m)
        total = total + scaled(xa, m, rest, 1, again)
        scale = inverse_rms(total)
        qk = aq[:, front] + jnp.dot(xg[1], wqkv[rows_of(rest), front], preferred_element_type=F32)
        qk = qk * scale
        qs[m] = rotated(qk[:, :HD])

        @pl.when(sec != 0)
        def _():
            ks[m] = rotated(qk[:, HD:].astype(BF).astype(F32))
            v = aq[:, back] + jnp.dot(
                xg[1], wqkv[rows_of(rest), back], preferred_element_type=F32
            )
            vs[m] = (v * scale).astype(BF)

        @pl.when(sec == 0)
        def _():
            turned = qk[:, HD:].astype(BF).astype(F32).T
            pairs = jnp.concatenate([turned[0:32, :], turned[32:64, :]], axis=1)
            kvs[m] = pairs.reshape(KV_HEADS, 4, 128)
            kvr[m, me] = kvs[m, kv_id]

            def send(k, carry):
                d = lax.rem(me + k, N)
                remote(
                    kvs.at[m, d // (HEADS // KV_HEADS)], kvr.at[m, me], S_KV, m, sec, d
                ).start()
                return carry

            lax.fori_loop(1, N, send, 0)

    def rotated(value):
        mid = HD // 2
        swapped = jnp.concatenate([value[:, mid:], value[:, :mid]], axis=1)
        return (value * cs[...] + swapped * sn[...]).astype(BF)

    def reduce_send(left, weights, phase, pass_phase, recv, m):
        def term(which, i):
            first = which * (D // 2) + i * 1024
            cols = pl.ds(pl.multiple_of(first, 1024), 1024)
            return jnp.dot(left, weights[:, cols], preferred_element_type=F32)

        def away(i, carry):
            value = term(rest, i).astype(BF)
            for j in range(8):
                pt[phase - S_RS1, m, i * 8 + j] = value[:, j * 128 : (j + 1) * 128]
            return carry

        lax.fori_loop(0, 2, away, 0)
        give = remote(pt.at[phase - S_RS1, m], dr.at[phase - S_RS1, m], pass_phase, m, sec, partner)
        give.start()

        def kept(i, carry):
            value = term(core, i)
            for j in range(8):
                own[i * 8 + j] = value[:, j * 128 : (j + 1) * 128]
            return carry

        lax.fori_loop(0, 2, kept, 0)
        give.wait()

        def add(j, carry):
            ps[phase - S_RS1, m, j] = (own[j] + dr[phase - S_RS1, m, j].astype(F32)).astype(BF)
            return carry

        lax.fori_loop(0, CHIPS, add, 0, unroll=4)
        others(
            lambda chip_to: remote(
                ps.at[phase - S_RS1, m, chip_to], recv.at[m, chip], phase, m, sec,
                chip_to * 2 + core,
            ).start()
        )
        recv[m, chip] = ps[phase - S_RS1, m, chip]

    def summed(recv, phase, m):
        received(recv.at[m, pl.ds(0, CHIPS - 1)], phase, m)
        total = recv[m, 0].astype(F32)
        for j in range(1, CHIPS):
            total = total + recv[m, j].astype(F32)
        return total

    def attend(m):
        @pl.when(sec == 0)
        def _():
            received(kvr.at[m, pl.ds(0, N - 1)], S_KV, m)
            both = kvr[m].reshape(HD, 128).T
            ks[m] = rotated(both[:LEN])
            vs[m] = both[LEN:].astype(BF)

        scores = lax.dot_general(qs[m], ks[m], nt, preferred_element_type=F32) * HD ** (-0.5)
        row = lax.broadcasted_iota(jnp.int32, (LEN, LEN), 0)
        col = lax.broadcasted_iota(jnp.int32, (LEN, LEN), 1)
        scores = jnp.where(row >= col, scores, -jnp.inf)
        top = jnp.max(scores, axis=-1, keepdims=True)
        e = jnp.exp(scores - top)
        prob = (e / jnp.sum(e, axis=-1, keepdims=True)).astype(BF)
        context = jnp.dot(prob, vs[m], preferred_element_type=F32)
        on = jnp.full((LEN, HD), heads[m, 0], jnp.int32) > me
        context = jnp.where(on, context, 0.0).astype(BF)
        reduce_send(context, wob, S_RS1, S_GIVE1, r1, m)

    def attended(m):
        value = xa[m, mine].astype(F32) + summed(r1, S_RS1, m)
        att[m] = value
        xb[m, mine] = value.astype(BF)
        gather_send(xb, S_AG2, m)

    def feed(m):
        received(xb.at[m, pl.ds(0, CHIPS - 1)], S_AG2, m)
        gather_pass(xb, S_PASS2, m)
        total = scaled(xb, m, core, 0, fgain)

        def first(i, carry):
            cols = pl.ds(pl.multiple_of(i * 256, 256), 256)
            acc[0, :, cols] = jnp.dot(
                xg[0], wgb[rows_of(core), cols], preferred_element_type=F32
            )
            acc[1, :, cols] = jnp.dot(
                xg[0], wub[rows_of(core), cols], preferred_element_type=F32
            )
            return carry

        lax.fori_loop(0, 2, first, 0)
        received(xb.at[m, pl.ds(0, CHIPS)], S_PASS2, m)
        scale = inverse_rms(total + scaled(xb, m, rest, 1, fgain))
        limit = jnp.full((LEN, 256), blocks[m, 0], jnp.int32) * BLOCK

        def second(i, carry):
            cols = pl.ds(pl.multiple_of(i * 256, 256), 256)
            gate = acc[0, :, cols] + jnp.dot(
                xg[1], wgb[rows_of(rest), cols], preferred_element_type=F32
            )
            up = acc[1, :, cols] + jnp.dot(
                xg[1], wub[rows_of(rest), cols], preferred_element_type=F32
            )
            gate, up = gate * scale, up * scale
            ids = me * UNITS + i * 256 + lax.broadcasted_iota(jnp.int32, (LEN, 256), 1)
            value = gate / (1.0 + jnp.exp(-gate)) * up
            hbuf[:, cols] = jnp.where(ids < limit, value, 0.0).astype(BF)
            return carry

        lax.fori_loop(0, 2, second, 0)
        reduce_send(hbuf[...], wdb, S_RS2, S_GIVE2, r2, m)

    def finish(m):
        yb[m] = (att[m] + summed(r2, S_RS2, m)).astype(BF)

        @pl.when(sec < SECTIONS - 1)
        def _():
            remote(yb.at[m], xa.at[m, mine], S_Y, m, sec + 1, me).start()

        @pl.when((sec == SECTIONS - 1) & (m < MICRO - 1))
        def _():
            pltpu.make_async_remote_copy(
                src_ref=yb.at[m], dst_ref=obuf.at[0, mine], send_sem=send_sem.at[S_Y, m],
                recv_sem=misc_sem.at[2], device_id=(m, me), device_id_type=MESH,
            ).start()

    def slot(i, carry):
        @pl.when(i < MICRO)
        def _():
            arrive(i)

        @pl.when((i < MICRO) & (sec == 0))
        def _():
            project(i)

        @pl.when(i == 0)
        def _():
            weight[3].wait()

        @pl.when(i == 1)
        def _():
            for w in weight[4:]:
                w.wait()

        @pl.when(i > 0)
        def _():
            feed(i - 1)

        @pl.when((i < MICRO) & (sec != 0))
        def _():
            project(i)

        @pl.when(i < MICRO)
        def _():
            attend(i)

        @pl.when(i > 0)
        def _():
            finish(i - 1)

        @pl.when(i < MICRO)
        def _():
            attended(i)

        return carry

    lax.fori_loop(0, MICRO + 1, slot, 0)

    @pl.when(sec == SECTIONS - 1)
    def _():
        obuf[0, mine] = yb[MICRO - 1]

    @pl.when(sec != SECTIONS - 1)
    def _():
        pltpu.make_async_copy(yb.at[0], yb.at[0], misc_sem.at[2]).wait()

    gather_send(obuf, S_AG3, 0)
    received(obuf.at[0, pl.ds(0, CHIPS - 1)], S_AG3, 0)
    gather_pass(obuf, S_PASS3, 0)
    near = pltpu.make_async_copy(
        obuf.at[0, half(core)], out.at[half(core)], misc_sem.at[3]
    )
    near.start()

    def drain(m, carry):
        @pl.when(sec != 0)
        def _():
            sent(xa.at[m, pl.ds(0, CHIPS - 1)], S_AG1, m)

        sent(xa.at[m, pl.ds(0, CHIPS)], S_PASS1, m)

        @pl.when(sec == 0)
        def _():
            sent(kvr.at[m, pl.ds(0, N - 1)], S_KV, m)

        sent(r1.at[m, pl.ds(0, CHIPS - 1)], S_RS1, m)
        sent(xb.at[m, pl.ds(0, CHIPS - 1)], S_AG2, m)
        sent(xb.at[m, pl.ds(0, CHIPS)], S_PASS2, m)
        sent(r2.at[m, pl.ds(0, CHIPS - 1)], S_RS2, m)

        @pl.when((sec < SECTIONS - 1) | (m < MICRO - 1))
        def _():
            sent(yb.at[m], S_Y, m)

        return carry

    lax.fori_loop(0, MICRO, drain, 0)

    @pl.when(sec != 0)
    def _():
        pltpu.make_async_copy(x0, x0, misc_sem.at[1]).wait()

    sent(obuf.at[0, pl.ds(0, CHIPS - 1)], S_AG3, 0)
    received(obuf.at[0, pl.ds(0, CHIPS)], S_PASS3, 0)
    far = pltpu.make_async_copy(obuf.at[0, half(rest)], out.at[half(rest)], misc_sem.at[4])
    far.start()
    sent(obuf.at[0, pl.ds(0, CHIPS)], S_PASS3, 0)
    near.wait()
    far.wait()


def tables():
    half = HD // 2
    frequency = ROPE_BASE ** (-(np.arange(half, dtype=np.float64) / half))
    angles = np.arange(LEN, dtype=np.float64)[:, None] * frequency[None, :]
    c, s = np.cos(angles).astype(np.float32), np.sin(angles).astype(np.float32)
    cs = np.concatenate([c, c], axis=1)
    sn = np.concatenate([-s, s], axis=1)
    pk = np.zeros((32, HD), np.float32)
    pv = np.zeros((32, HD), np.float32)
    tk = np.zeros((64, 32), np.float32)
    tv = np.zeros((64, 32), np.float32)
    for j in range(4):
        for k in range(KV_HEADS):
            pk[j * KV_HEADS + k, k * 4 + j] = 1.0
            pv[j * KV_HEADS + k, 32 + k * 4 + j] = 1.0
            tk[k * 8 + j, j * KV_HEADS + k] = 1.0
            tv[k * 8 + 4 + j, j * KV_HEADS + k] = 1.0
    order = np.zeros((2 * HD, 2 * HD), np.float32)
    for c in range(2):
        for q in range(CHIPS):
            for r in range(4):
                row, col = (c * CHIPS + q) * 8 + r, 4 * (2 * q + c) + r
                order[row, col] = 1.0
                order[row + 4, HD + col] = 1.0
    return (jnp.asarray(cs), jnp.asarray(sn)) + tuple(
        jnp.asarray(a, BF) for a in (pk, pv, tk, tv, order)
    )


def per_device(*args):
    any_spec = pl.BlockSpec(memory_space=pl.ANY)
    vmem = pl.BlockSpec(memory_space=pltpu.VMEM)
    smem = pl.BlockSpec(memory_space=pltpu.SMEM)
    piece = (LEN, 128)
    gathered = pl.pallas_call(
        body,
        out_shape=jax.ShapeDtypeStruct((N, *piece), BF),
        in_specs=[
            any_spec, vmem, any_spec, any_spec, any_spec, any_spec, vmem, any_spec, any_spec,
            any_spec, smem, smem, vmem, vmem, vmem, vmem, vmem, vmem, vmem,
        ],
        out_specs=any_spec,
        scratch_shapes=[
            pltpu.VMEM((CHIPS, *piece), BF),
            pltpu.VMEM((MICRO, N, *piece), BF),
            pltpu.VMEM((MICRO, N, *piece), BF),
            pltpu.VMEM((MICRO, CHIPS, *piece), BF),
            pltpu.VMEM((MICRO, CHIPS, *piece), BF),
            pltpu.VMEM((2, MICRO, CHIPS, *piece), BF),
            pltpu.VMEM((2, MICRO, CHIPS, *piece), BF),
            pltpu.VMEM((2, MICRO, CHIPS, *piece), BF),
            pltpu.VMEM((CHIPS, *piece), F32),
            pltpu.VMEM((MICRO, KV_HEADS, 4, 128), F32),
            pltpu.VMEM((MICRO, N, 4, 128), F32),
            pltpu.VMEM((1, N, *piece), BF),
            pltpu.VMEM((MICRO, *piece), BF),
            pltpu.VMEM((MICRO, *piece), F32),
            pltpu.VMEM((2, LEN, D // 2), BF),
            pltpu.VMEM((2, LEN, UNITS), F32),
            pltpu.VMEM((LEN, UNITS), BF),
            pltpu.VMEM((MICRO, *piece), BF),
            pltpu.VMEM((MICRO, *piece), BF),
            pltpu.VMEM((MICRO, *piece), BF),
            pltpu.VMEM((LEN, 3 * HD), F32),
            pltpu.VMEM((KV_HEADS, 8, D), BF),
            pltpu.VMEM((N, 8, D), BF),
            pltpu.VMEM((D, 3 * HD), BF),
            pltpu.VMEM((D, 32), BF),
            pltpu.VMEM((D, 32), BF),
            pltpu.VMEM((HD, D), BF),
            pltpu.VMEM((D, UNITS), BF),
            pltpu.VMEM((D, UNITS), BF),
            pltpu.VMEM((UNITS, D), BF),
            pltpu.SemaphoreType.DMA((14, MICRO)),
            pltpu.SemaphoreType.DMA((14, MICRO)),
            pltpu.SemaphoreType.DMA((5,)),
            pltpu.SemaphoreType.DMA((7,)),
        ],
        compiler_params=pltpu.CompilerParams(
            collective_id=0, has_side_effects=True, vmem_limit_bytes=56 * 1024 * 1024
        ),
    )(*args, *tables())
    return gathered.transpose(1, 0, 2).reshape(1, 1, LEN, D)


def solution(mesh):
    return jax.shard_map(
        per_device,
        mesh=mesh,
        in_specs=(
            P(None, "section", None, None),
            P("section", None),
            P("section", None, "mp"),
            P("section", None, "mp"),
            P("section", None, "mp"),
            P("section", "mp", None),
            P("section", None),
            P("section", None, "mp"),
            P("section", None, "mp"),
            P("section", "mp", None),
            P(None, "section"),
            P(None, "section"),
        ),
        out_specs=P(None, "section", None, None),
        check_vma=False,
    )
```

```python
import functools

import jax
import jax.numpy as jnp
import numpy as np
from jax import lax
from jax.experimental import pallas as pl
from jax.experimental.pallas import tpu as pltpu
from jax.sharding import PartitionSpec as P

HEADS = 32
KV_HEADS = 8
HD = 128
BLOCK = 128
D = 4096
LEN = 64
N = 32
UNITS = 512
MICRO = 4
SECTIONS = 4
ROPE_BASE = 500000.0
EPSILON = 1e-05
MESH = pl.DeviceIdType.MESH
BF = jnp.bfloat16
F32 = jnp.float32
CHIPS = 16
(
    S_IN, S_Y, S_AG1, S_PASS1, S_KV, S_GIVE1, S_RS1, S_RS2, S_AG2, S_PASS2, S_GIVE2, S_AG3, S_PASS3,
    S_W,
) = range(14)
ORDERS = (
    "P0P1T0P2T1C0T2P3C1D0C2D1E0T3D2E1C3E2D3E3",
    "A0P0A1T0A2P1T1C0P2T2C1A3D0C2D1P3E0T3D2E1C3E2D3E3",
    "A0P0A1T0A2P1T1C0P2T2A3C1D0C2P3T3D1E0C3D2E1D3E2E3",
    "A0A1P0T0P1A2T1A3C0P2T2C1P3T3C2D0C3D1D2D3E0E1E2E3",
)
STEPS, PACK = 24, 6


def packed(order):
    codes = ["APTCDE".index(a) * MICRO + int(b) for a, b in zip(order[::2], order[1::2])]
    codes += [SKIP] * (STEPS - len(codes))
    return [
        sum(c << (5 * i) for i, c in enumerate(codes[k : k + PACK]))
        for k in range(0, STEPS, PACK)
    ]


SKIP = 24
WORDS = [packed(order) for order in ORDERS]
RING = (0, 1, 2, 1)
FAR_FIRST = sorted(
    [(dx, dz) for dx in range(4) for dz in range(4) if (dx, dz) != (0, 0)],
    key=lambda d: -(RING[d[0]] + RING[d[1]]),
)


def body(
    hid, again, wq, wk, wv, wo, fgain, wg, wu, wd, blocks, heads,
    cs, sn, pk, pv, tk, tv, order,
    out,
    x0, xa, xb, r1, r2, pt, ps, dr, own, kvs, kvr, obuf, yb, att, xg, acc, hbuf, qs,
    ks, vs, aq, wgive, wtake, wqkv, wkb, wvb, wob, wgb, wub, wdb,
    send_sem, recv_sem, misc_sem, w_sem,
):
    sec = lax.axis_index("section")
    me = lax.axis_index("mp")
    chip = me // 2
    core = lax.rem(me, 2)
    rest = 1 - core
    partner = chip * 2 + rest
    mine = core * CHIPS + chip
    kv_id = me // (HEADS // KV_HEADS)
    at_x, at_z = chip // 4, lax.rem(chip, 4)

    def others(fn):
        for dx, dz in FAR_FIRST:
            fn(lax.rem(at_x + dx, 4) * 4 + lax.rem(at_z + dz, 4))

    def remote(src, dst, phase, m, s, d):
        return pltpu.make_async_remote_copy(
            src_ref=src, dst_ref=dst, send_sem=send_sem.at[phase, m],
            recv_sem=recv_sem.at[phase, m], device_id=(s, d), device_id_type=MESH,
        )

    def received(view, phase, m):
        pltpu.make_async_copy(view, view, recv_sem.at[phase, m]).wait()

    def sent(view, phase, m):
        pltpu.make_async_copy(view, view, send_sem.at[phase, m]).wait()

    def half(which):
        return pl.ds(pl.multiple_of(which * CHIPS, CHIPS), CHIPS)

    loads = [
        (wk.at[0], wkb),
        (wv.at[0], wvb),
        (wq.at[0], wqkv.at[:, pl.ds(0, HD)]),
        (wo.at[0], wob),
        (wg.at[0], wgb),
        (wu.at[0], wub),
        (wd.at[0], wdb),
    ]
    weight = [pltpu.make_async_copy(s, d, w_sem.at[i]) for i, (s, d) in enumerate(loads)]

    def load_hidden(dst, first, sem):
        def step(j, carry):
            cols = pl.ds(pl.multiple_of((core * CHIPS + j) * 128, 128), 128)
            pltpu.make_async_copy(hid.at[0, 0, :, cols], dst.at[first + j], sem).start()
            return carry

        lax.fori_loop(0, CHIPS, step, 0)

    @pl.when(sec == 0)
    def _():
        load_hidden(xa.at[0], core * CHIPS, recv_sem.at[S_IN, 0])

    @pl.when(sec != 0)
    def _():
        load_hidden(x0, 0, misc_sem.at[0])

    for w in weight:
        w.start()

    barrier = pltpu.get_barrier_semaphore()

    def greet(k, carry):
        pl.semaphore_signal(
            barrier, inc=1, device_id=(sec, lax.rem(me + k, N)), device_id_type=MESH
        )
        return carry

    lax.fori_loop(1, N, greet, 0)
    for k in range(1, SECTIONS):
        pl.semaphore_signal(
            barrier, inc=1, device_id=(lax.rem(sec + k, SECTIONS), me), device_id_type=MESH
        )

    weight[0].wait()
    weight[1].wait()
    nt = (((1,), (1,)), ((), ()))

    def permute_rows(i, carry):
        rows = pl.ds(pl.multiple_of(i * 512, 512), 512)
        both = jnp.dot(wkb[rows, :], pk[...], preferred_element_type=F32) + jnp.dot(
            wvb[rows, :], pv[...], preferred_element_type=F32
        )
        wqkv[rows, pl.ds(HD, HD)] = both.astype(BF)
        return carry

    def turn_rows(i, carry):
        rows = pl.ds(pl.multiple_of(i * 512, 512), 512)
        both = lax.dot_general(
            tk[...], wkb[rows, :], nt, preferred_element_type=F32
        ) + lax.dot_general(tv[...], wvb[rows, :], nt, preferred_element_type=F32)
        wgive[:, :, rows] = both.reshape(KV_HEADS, 8, 512).astype(BF)
        return carry

    @pl.when(sec == 0)
    def _():
        lax.fori_loop(0, D // 512, permute_rows, 0)

    @pl.when(sec != 0)
    def _():
        lax.fori_loop(0, D // 512, turn_rows, 0)

    pl.semaphore_wait(barrier, N - 1 + SECTIONS - 1)

    @pl.when(sec != 0)
    def _():
        pltpu.make_async_copy(x0, x0, misc_sem.at[0]).wait()
        pltpu.make_async_remote_copy(
            src_ref=x0, dst_ref=xa.at[sec, half(core)], send_sem=misc_sem.at[1],
            recv_sem=recv_sem.at[S_IN, sec], device_id=(0, me), device_id_type=MESH,
        ).start()
        others(
            lambda chip_to: remote(
                wgive.at[chip_to // 2], wtake.at[mine], S_W, 0, sec, chip_to * 2 + core
            ).start()
        )
        wtake[mine] = wgive[chip // 2]
        received(wtake.at[pl.ds(0, CHIPS - 1)], S_W, 0)
        view = wtake.at[half(core)]
        swap = remote(view, view, S_W, 1, sec, partner)
        swap.start()
        swap.wait()

        def put_in_order(i, carry):
            rows = pl.ds(pl.multiple_of(i * 512, 512), 512)
            chunk = wtake[:, :, rows].astype(F32).reshape(2 * HD, 512).T.astype(BF)
            wqkv[rows, pl.ds(HD, 2 * HD)] = jnp.dot(
                chunk, order[...], preferred_element_type=F32
            ).astype(BF)
            return carry

        lax.fori_loop(0, D // 512, put_in_order, 0)
        sent(wtake.at[pl.ds(0, CHIPS - 1)], S_W, 0)

    weight[2].wait()

    def gather_send(buf, phase, m):
        view = buf.at[m, mine]
        others(lambda chip_to: remote(view, view, phase, m, sec, chip_to * 2 + core).start())

    def gather_pass(buf, phase, m):
        view = buf.at[m, half(core)]
        remote(view, view, phase, m, sec, partner).start()

    def scaled(buf, m, which, slot, gain):
        total = jnp.zeros((LEN, 128), F32)
        for j in range(CHIPS):
            block = which * CHIPS + j
            value = buf[m, block].astype(F32)
            total = total + value * value
            factor = gain[:, pl.ds(pl.multiple_of(block * 128, 128), 128)].astype(F32)
            xg[slot, :, j * 128 : (j + 1) * 128] = (value * factor).astype(BF)
        return total

    def inverse_rms(total):
        mean_sq = jnp.sum(total, axis=-1, keepdims=True) * (1.0 / D)
        return lax.rsqrt(mean_sq + EPSILON)

    def rows_of(which):
        return pl.ds(pl.multiple_of(which * (D // 2), D // 2), D // 2)

    def arrive(m):
        @pl.when(sec != 0)
        def _():
            received(yb.at[m], S_Y, m)
            gather_send(xa, S_AG1, m)

    def project(m):
        @pl.when(sec == 0)
        def _():
            received(xa.at[m, pl.ds(0, CHIPS)], S_IN, m)

        @pl.when(sec != 0)
        def _():
            received(xa.at[m, pl.ds(0, CHIPS - 1)], S_AG1, m)

        gather_pass(xa, S_PASS1, m)
        total = scaled(xa, m, core, 0, again)
        front, back = pl.ds(0, 2 * HD), pl.ds(2 * HD, HD)
        aq[:, front] = jnp.dot(xg[0], wqkv[rows_of(core), front], preferred_element_type=F32)

        @pl.when(sec != 0)
        def _():
            aq[:, back] = jnp.dot(xg[0], wqkv[rows_of(core), back], preferred_element_type=F32)

        received(xa.at[m, pl.ds(0, CHIPS)], S_PASS1, m)
        total = total + scaled(xa, m, rest, 1, again)
        scale = inverse_rms(total)
        qk = aq[:, front] + jnp.dot(xg[1], wqkv[rows_of(rest), front], preferred_element_type=F32)
        qk = qk * scale
        qs[m] = rotated(qk[:, :HD])

        @pl.when(sec != 0)
        def _():
            ks[m] = rotated(qk[:, HD:].astype(BF).astype(F32))
            v = aq[:, back] + jnp.dot(
                xg[1], wqkv[rows_of(rest), back], preferred_element_type=F32
            )
            vs[m] = (v * scale).astype(BF)

        @pl.when(sec == 0)
        def _():
            turned = qk[:, HD:].astype(BF).astype(F32).T
            pairs = jnp.concatenate([turned[0:32, :], turned[32:64, :]], axis=1)
            kvs[m] = pairs.reshape(KV_HEADS, 4, 128)
            kvr[m, me] = kvs[m, kv_id]

            def send(k, carry):
                d = lax.rem(me + k, N)
                remote(
                    kvs.at[m, d // (HEADS // KV_HEADS)], kvr.at[m, me], S_KV, m, sec, d
                ).start()
                return carry

            lax.fori_loop(1, N, send, 0)

    def rotated(value):
        mid = HD // 2
        swapped = jnp.concatenate([value[:, mid:], value[:, :mid]], axis=1)
        return (value * cs[...] + swapped * sn[...]).astype(BF)

    def reduce_send(left, weights, phase, pass_phase, recv, m):
        def term(which, i):
            first = which * (D // 2) + i * 1024
            cols = pl.ds(pl.multiple_of(first, 1024), 1024)
            return jnp.dot(left, weights[:, cols], preferred_element_type=F32)

        def away(i, carry):
            value = term(rest, i).astype(BF)
            for j in range(8):
                pt[phase - S_RS1, m, i * 8 + j] = value[:, j * 128 : (j + 1) * 128]
            return carry

        lax.fori_loop(0, 2, away, 0)
        give = remote(pt.at[phase - S_RS1, m], dr.at[phase - S_RS1, m], pass_phase, m, sec, partner)
        give.start()

        def kept(i, carry):
            value = term(core, i)
            for j in range(8):
                own[i * 8 + j] = value[:, j * 128 : (j + 1) * 128]
            return carry

        lax.fori_loop(0, 2, kept, 0)
        give.wait()

        def add(j, carry):
            ps[phase - S_RS1, m, j] = (own[j] + dr[phase - S_RS1, m, j].astype(F32)).astype(BF)
            return carry

        lax.fori_loop(0, CHIPS, add, 0, unroll=4)
        others(
            lambda chip_to: remote(
                ps.at[phase - S_RS1, m, chip_to], recv.at[m, chip], phase, m, sec,
                chip_to * 2 + core,
            ).start()
        )
        recv[m, chip] = ps[phase - S_RS1, m, chip]

    def summed(recv, phase, m):
        received(recv.at[m, pl.ds(0, CHIPS - 1)], phase, m)
        total = recv[m, 0].astype(F32)
        for j in range(1, CHIPS):
            total = total + recv[m, j].astype(F32)
        return total

    def attend(m):
        @pl.when(sec == 0)
        def _():
            received(kvr.at[m, pl.ds(0, N - 1)], S_KV, m)
            both = kvr[m].reshape(HD, 128).T
            ks[m] = rotated(both[:LEN])
            vs[m] = both[LEN:].astype(BF)

        scores = lax.dot_general(qs[m], ks[m], nt, preferred_element_type=F32) * HD ** (-0.5)
        row = lax.broadcasted_iota(jnp.int32, (LEN, LEN), 0)
        col = lax.broadcasted_iota(jnp.int32, (LEN, LEN), 1)
        scores = jnp.where(row >= col, scores, -jnp.inf)
        top = jnp.max(scores, axis=-1, keepdims=True)
        e = jnp.exp(scores - top)
        prob = (e / jnp.sum(e, axis=-1, keepdims=True)).astype(BF)
        context = jnp.dot(prob, vs[m], preferred_element_type=F32)
        on = jnp.full((LEN, HD), heads[m, 0], jnp.int32) > me
        context = jnp.where(on, context, 0.0).astype(BF)
        reduce_send(context, wob, S_RS1, S_GIVE1, r1, m)

    def attended(m):
        value = xa[m, mine].astype(F32) + summed(r1, S_RS1, m)
        att[m] = value
        xb[m, mine] = value.astype(BF)
        gather_send(xb, S_AG2, m)

    def feed(m):
        received(xb.at[m, pl.ds(0, CHIPS - 1)], S_AG2, m)
        gather_pass(xb, S_PASS2, m)
        total = scaled(xb, m, core, 0, fgain)

        def first(i, carry):
            cols = pl.ds(pl.multiple_of(i * 256, 256), 256)
            acc[0, :, cols] = jnp.dot(
                xg[0], wgb[rows_of(core), cols], preferred_element_type=F32
            )
            acc[1, :, cols] = jnp.dot(
                xg[0], wub[rows_of(core), cols], preferred_element_type=F32
            )
            return carry

        lax.fori_loop(0, 2, first, 0)
        received(xb.at[m, pl.ds(0, CHIPS)], S_PASS2, m)
        scale = inverse_rms(total + scaled(xb, m, rest, 1, fgain))
        limit = jnp.full((LEN, 256), blocks[m, 0], jnp.int32) * BLOCK

        def second(i, carry):
            cols = pl.ds(pl.multiple_of(i * 256, 256), 256)
            gate = acc[0, :, cols] + jnp.dot(
                xg[1], wgb[rows_of(rest), cols], preferred_element_type=F32
            )
            up = acc[1, :, cols] + jnp.dot(
                xg[1], wub[rows_of(rest), cols], preferred_element_type=F32
            )
            gate, up = gate * scale, up * scale
            ids = me * UNITS + i * 256 + lax.broadcasted_iota(jnp.int32, (LEN, 256), 1)
            value = gate / (1.0 + jnp.exp(-gate)) * up
            hbuf[:, cols] = jnp.where(ids < limit, value, 0.0).astype(BF)
            return carry

        lax.fori_loop(0, 2, second, 0)
        reduce_send(hbuf[...], wdb, S_RS2, S_GIVE2, r2, m)

    def finish(m):
        yb[m] = (att[m] + summed(r2, S_RS2, m)).astype(BF)

        @pl.when(sec < SECTIONS - 1)
        def _():
            remote(yb.at[m], xa.at[m, mine], S_Y, m, sec + 1, me).start()

        @pl.when((sec == SECTIONS - 1) & (m < MICRO - 1))
        def _():
            pltpu.make_async_remote_copy(
                src_ref=yb.at[m], dst_ref=obuf.at[0, mine], send_sem=send_sem.at[S_Y, m],
                recv_sem=misc_sem.at[2], device_id=(m, me), device_id_type=MESH,
            ).start()

    work = (arrive, project, attend, attended, feed, finish)
    waits = {2: weight[3:4], 4: weight[4:]}

    def step(t, carry):
        word = jnp.int32(0)
        for s in range(SECTIONS):
            for k in range(STEPS // PACK):
                here = (sec == s) & (t // PACK == k)
                word = jnp.where(here, jnp.int32(WORDS[s][k]), word)
        for k in range(PACK - 1):
            word = jnp.where(lax.rem(t, PACK) > k, word // 32, word)
        code = lax.rem(word, 32)
        kind, m = code // MICRO, lax.rem(code, MICRO)
        for i, fn in enumerate(work):
            @pl.when(kind == i)
            def _():
                if i in waits:
                    @pl.when(m == 0)
                    def _():
                        for w in waits[i]:
                            w.wait()

                fn(m)

        return carry

    lax.fori_loop(0, STEPS, step, 0)

    @pl.when(sec == SECTIONS - 1)
    def _():
        obuf[0, mine] = yb[MICRO - 1]

    @pl.when(sec != SECTIONS - 1)
    def _():
        pltpu.make_async_copy(yb.at[0], yb.at[0], misc_sem.at[2]).wait()

    gather_send(obuf, S_AG3, 0)
    received(obuf.at[0, pl.ds(0, CHIPS - 1)], S_AG3, 0)
    gather_pass(obuf, S_PASS3, 0)
    near = pltpu.make_async_copy(
        obuf.at[0, half(core)], out.at[half(core)], misc_sem.at[3]
    )
    near.start()

    def drain(m, carry):
        @pl.when(sec != 0)
        def _():
            sent(xa.at[m, pl.ds(0, CHIPS - 1)], S_AG1, m)

        sent(xa.at[m, pl.ds(0, CHIPS)], S_PASS1, m)

        @pl.when(sec == 0)
        def _():
            sent(kvr.at[m, pl.ds(0, N - 1)], S_KV, m)

        sent(r1.at[m, pl.ds(0, CHIPS - 1)], S_RS1, m)
        sent(xb.at[m, pl.ds(0, CHIPS - 1)], S_AG2, m)
        sent(xb.at[m, pl.ds(0, CHIPS)], S_PASS2, m)
        sent(r2.at[m, pl.ds(0, CHIPS - 1)], S_RS2, m)

        @pl.when((sec < SECTIONS - 1) | (m < MICRO - 1))
        def _():
            sent(yb.at[m], S_Y, m)

        return carry

    lax.fori_loop(0, MICRO, drain, 0)

    @pl.when(sec != 0)
    def _():
        pltpu.make_async_copy(x0, x0, misc_sem.at[1]).wait()

    sent(obuf.at[0, pl.ds(0, CHIPS - 1)], S_AG3, 0)
    received(obuf.at[0, pl.ds(0, CHIPS)], S_PASS3, 0)
    far = pltpu.make_async_copy(obuf.at[0, half(rest)], out.at[half(rest)], misc_sem.at[4])
    far.start()
    sent(obuf.at[0, pl.ds(0, CHIPS)], S_PASS3, 0)
    near.wait()
    far.wait()


def tables():
    half = HD // 2
    frequency = ROPE_BASE ** (-(np.arange(half, dtype=np.float64) / half))
    angles = np.arange(LEN, dtype=np.float64)[:, None] * frequency[None, :]
    c, s = np.cos(angles).astype(np.float32), np.sin(angles).astype(np.float32)
    cs = np.concatenate([c, c], axis=1)
    sn = np.concatenate([-s, s], axis=1)
    pk = np.zeros((32, HD), np.float32)
    pv = np.zeros((32, HD), np.float32)
    tk = np.zeros((64, 32), np.float32)
    tv = np.zeros((64, 32), np.float32)
    for j in range(4):
        for k in range(KV_HEADS):
            pk[j * KV_HEADS + k, k * 4 + j] = 1.0
            pv[j * KV_HEADS + k, 32 + k * 4 + j] = 1.0
            tk[k * 8 + j, j * KV_HEADS + k] = 1.0
            tv[k * 8 + 4 + j, j * KV_HEADS + k] = 1.0
    order = np.zeros((2 * HD, 2 * HD), np.float32)
    for c in range(2):
        for q in range(CHIPS):
            for r in range(4):
                row, col = (c * CHIPS + q) * 8 + r, 4 * (2 * q + c) + r
                order[row, col] = 1.0
                order[row + 4, HD + col] = 1.0
    return (jnp.asarray(cs), jnp.asarray(sn)) + tuple(
        jnp.asarray(a, BF) for a in (pk, pv, tk, tv, order)
    )


def per_device(*args):
    any_spec = pl.BlockSpec(memory_space=pl.ANY)
    vmem = pl.BlockSpec(memory_space=pltpu.VMEM)
    smem = pl.BlockSpec(memory_space=pltpu.SMEM)
    piece = (LEN, 128)
    gathered = pl.pallas_call(
        body,
        out_shape=jax.ShapeDtypeStruct((N, *piece), BF),
        in_specs=[
            any_spec, vmem, any_spec, any_spec, any_spec, any_spec, vmem, any_spec, any_spec,
            any_spec, smem, smem, vmem, vmem, vmem, vmem, vmem, vmem, vmem,
        ],
        out_specs=any_spec,
        scratch_shapes=[
            pltpu.VMEM((CHIPS, *piece), BF),
            pltpu.VMEM((MICRO, N, *piece), BF),
            pltpu.VMEM((MICRO, N, *piece), BF),
            pltpu.VMEM((MICRO, CHIPS, *piece), BF),
            pltpu.VMEM((MICRO, CHIPS, *piece), BF),
            pltpu.VMEM((2, MICRO, CHIPS, *piece), BF),
            pltpu.VMEM((2, MICRO, CHIPS, *piece), BF),
            pltpu.VMEM((2, MICRO, CHIPS, *piece), BF),
            pltpu.VMEM((CHIPS, *piece), F32),
            pltpu.VMEM((MICRO, KV_HEADS, 4, 128), F32),
            pltpu.VMEM((MICRO, N, 4, 128), F32),
            pltpu.VMEM((1, N, *piece), BF),
            pltpu.VMEM((MICRO, *piece), BF),
            pltpu.VMEM((MICRO, *piece), F32),
            pltpu.VMEM((2, LEN, D // 2), BF),
            pltpu.VMEM((2, LEN, UNITS), F32),
            pltpu.VMEM((LEN, UNITS), BF),
            pltpu.VMEM((MICRO, *piece), BF),
            pltpu.VMEM((MICRO, *piece), BF),
            pltpu.VMEM((MICRO, *piece), BF),
            pltpu.VMEM((LEN, 3 * HD), F32),
            pltpu.VMEM((KV_HEADS, 8, D), BF),
            pltpu.VMEM((N, 8, D), BF),
            pltpu.VMEM((D, 3 * HD), BF),
            pltpu.VMEM((D, 32), BF),
            pltpu.VMEM((D, 32), BF),
            pltpu.VMEM((HD, D), BF),
            pltpu.VMEM((D, UNITS), BF),
            pltpu.VMEM((D, UNITS), BF),
            pltpu.VMEM((UNITS, D), BF),
            pltpu.SemaphoreType.DMA((14, MICRO)),
            pltpu.SemaphoreType.DMA((14, MICRO)),
            pltpu.SemaphoreType.DMA((5,)),
            pltpu.SemaphoreType.DMA((7,)),
        ],
        compiler_params=pltpu.CompilerParams(
            collective_id=0, has_side_effects=True, vmem_limit_bytes=56 * 1024 * 1024
        ),
    )(*args, *tables())
    return gathered.transpose(1, 0, 2).reshape(1, 1, LEN, D)


def solution(mesh):
    return jax.shard_map(
        per_device,
        mesh=mesh,
        in_specs=(
            P(None, "section", None, None),
            P("section", None),
            P("section", None, "mp"),
            P("section", None, "mp"),
            P("section", None, "mp"),
            P("section", "mp", None),
            P("section", None),
            P("section", None, "mp"),
            P("section", None, "mp"),
            P("section", "mp", None),
            P(None, "section"),
            P(None, "section"),
        ),
        out_specs=P(None, "section", None, None),
        check_vma=False,
    )
```

```python
import functools

import jax
import jax.numpy as jnp
import numpy as np
from jax import lax
from jax.experimental import pallas as pl
from jax.experimental.pallas import tpu as pltpu
from jax.sharding import PartitionSpec as P

HEADS = 32
KV_HEADS = 8
HD = 128
BLOCK = 128
D = 4096
LEN = 64
N = 32
UNITS = 512
MICRO = 4
SECTIONS = 4
ROPE_BASE = 500000.0
EPSILON = 1e-05
MESH = pl.DeviceIdType.MESH
BF = jnp.bfloat16
F32 = jnp.float32
CHIPS = 16
(
    S_IN, S_Y, S_AG1, S_PASS1, S_KV, S_GIVE1, S_RS1, S_RS2, S_AG2, S_PASS2, S_GIVE2, S_AG3, S_PASS3,
    S_W,
) = range(14)
ORDERS = (
    "P0P1T0P2T1C0T2P3C1D0C2D1E0T3D2E1C3E2D3E3",
    "A0P0A1T0A2P1T1C0P2T2C1A3D0C2D1P3E0T3D2E1C3E2D3E3",
    "A0P0A1T0A2P1T1C0P2T2A3C1D0C2P3T3D1E0C3D2E1D3E2E3",
    "A0A1P0T0P1A2T1A3C0P2T2C1P3T3C2D0C3D1D2D3E0E1E2E3",
)
STEPS, PACK = 24, 6


def packed(order):
    codes = ["APTCDE".index(a) * MICRO + int(b) for a, b in zip(order[::2], order[1::2])]
    codes += [SKIP] * (STEPS - len(codes))
    return [
        sum(c << (5 * i) for i, c in enumerate(codes[k : k + PACK]))
        for k in range(0, STEPS, PACK)
    ]


SKIP = 24
WORDS = [packed(order) for order in ORDERS]
RING = (0, 1, 2, 1)
FAR_FIRST = sorted(
    [(dx, dz) for dx in range(4) for dz in range(4) if (dx, dz) != (0, 0)],
    key=lambda d: -(RING[d[0]] + RING[d[1]]),
)


def body(
    hid, again, wq, wk, wv, wo, fgain, wg, wu, wd, blocks, heads,
    cs, sn, pk, pv, tk, tv, order,
    out,
    x0, xa, xb, r1, r2, pt, ps, dr, own, kvs, kvr, obuf, yb, att, xg, acc, hbuf, qs,
    ks, vs, aq, wgive, wtake, wqkv, wkb, wvb, wob, wgb, wub, wdb,
    send_sem, recv_sem, misc_sem, w_sem,
):
    sec = lax.axis_index("section")
    me = lax.axis_index("mp")
    chip = me // 2
    core = lax.rem(me, 2)
    rest = 1 - core
    partner = chip * 2 + rest
    mine = core * CHIPS + chip
    kv_id = me // (HEADS // KV_HEADS)
    at_x, at_z = chip // 4, lax.rem(chip, 4)

    def others(fn):
        for dx, dz in FAR_FIRST:
            fn(lax.rem(at_x + dx, 4) * 4 + lax.rem(at_z + dz, 4))

    def remote(src, dst, phase, m, s, d):
        return pltpu.make_async_remote_copy(
            src_ref=src, dst_ref=dst, send_sem=send_sem.at[phase, m],
            recv_sem=recv_sem.at[phase, m], device_id=(s, d), device_id_type=MESH,
        )

    def received(view, phase, m):
        pltpu.make_async_copy(view, view, recv_sem.at[phase, m]).wait()

    def sent(view, phase, m):
        pltpu.make_async_copy(view, view, send_sem.at[phase, m]).wait()

    def half(which):
        return pl.ds(pl.multiple_of(which * CHIPS, CHIPS), CHIPS)

    loads = [
        (wk.at[0], wkb),
        (wv.at[0], wvb),
        (wq.at[0], wqkv.at[:, pl.ds(0, HD)]),
        (wo.at[0], wob),
        (wg.at[0], wgb),
        (wu.at[0], wub),
        (wd.at[0], wdb),
    ]
    weight = [pltpu.make_async_copy(s, d, w_sem.at[i]) for i, (s, d) in enumerate(loads)]

    def load_hidden(dst, first, sem):
        def step(j, carry):
            cols = pl.ds(pl.multiple_of((core * CHIPS + j) * 128, 128), 128)
            pltpu.make_async_copy(hid.at[0, 0, :, cols], dst.at[first + j], sem).start()
            return carry

        lax.fori_loop(0, CHIPS, step, 0)

    @pl.when(sec == 0)
    def _():
        load_hidden(xa.at[0], core * CHIPS, recv_sem.at[S_IN, 0])

    @pl.when(sec != 0)
    def _():
        load_hidden(x0, 0, misc_sem.at[0])

    for w in weight:
        w.start()

    barrier = pltpu.get_barrier_semaphore()

    def greet(k, carry):
        pl.semaphore_signal(
            barrier, inc=1, device_id=(sec, lax.rem(me + k, N)), device_id_type=MESH
        )
        return carry

    lax.fori_loop(1, N, greet, 0)
    for k in range(1, SECTIONS):
        pl.semaphore_signal(
            barrier, inc=1, device_id=(lax.rem(sec + k, SECTIONS), me), device_id_type=MESH
        )

    weight[0].wait()
    weight[1].wait()
    nt = (((1,), (1,)), ((), ()))

    def permute_rows(i, carry):
        rows = pl.ds(pl.multiple_of(i * 512, 512), 512)
        both = jnp.dot(wkb[rows, :], pk[...], preferred_element_type=F32) + jnp.dot(
            wvb[rows, :], pv[...], preferred_element_type=F32
        )
        wqkv[rows, pl.ds(HD, HD)] = both.astype(BF)
        return carry

    def turn_rows(i, carry):
        rows = pl.ds(pl.multiple_of(i * 512, 512), 512)
        both = lax.dot_general(
            tk[...], wkb[rows, :], nt, preferred_element_type=F32
        ) + lax.dot_general(tv[...], wvb[rows, :], nt, preferred_element_type=F32)
        wgive[:, :, rows] = both.reshape(KV_HEADS, 8, 512).astype(BF)
        return carry

    @pl.when(sec == 0)
    def _():
        lax.fori_loop(0, D // 512, permute_rows, 0)

    @pl.when(sec != 0)
    def _():
        lax.fori_loop(0, D // 512, turn_rows, 0)

    pl.semaphore_wait(barrier, N - 1 + SECTIONS - 1)

    @pl.when(sec != 0)
    def _():
        pltpu.make_async_copy(x0, x0, misc_sem.at[0]).wait()
        pltpu.make_async_remote_copy(
            src_ref=x0, dst_ref=xa.at[sec, half(core)], send_sem=misc_sem.at[1],
            recv_sem=recv_sem.at[S_IN, sec], device_id=(0, me), device_id_type=MESH,
        ).start()
        others(
            lambda chip_to: remote(
                wgive.at[chip_to // 2], wtake.at[mine], S_W, 0, sec, chip_to * 2 + core
            ).start()
        )
        wtake[mine] = wgive[chip // 2]
        received(wtake.at[pl.ds(0, CHIPS - 1)], S_W, 0)
        view = wtake.at[half(core)]
        swap = remote(view, view, S_W, 1, sec, partner)
        swap.start()
        swap.wait()

        def put_in_order(i, carry):
            rows = pl.ds(pl.multiple_of(i * 512, 512), 512)
            chunk = wtake[:, :, rows].astype(F32).reshape(2 * HD, 512).T.astype(BF)
            wqkv[rows, pl.ds(HD, 2 * HD)] = jnp.dot(
                chunk, order[...], preferred_element_type=F32
            ).astype(BF)
            return carry

        lax.fori_loop(0, D // 512, put_in_order, 0)
        sent(wtake.at[pl.ds(0, CHIPS - 1)], S_W, 0)

    weight[2].wait()

    def gather_send(buf, phase, m):
        view = buf.at[m, mine]
        others(lambda chip_to: remote(view, view, phase, m, sec, chip_to * 2 + core).start())

    def gather_pass(buf, phase, m):
        view = buf.at[m, half(core)]
        remote(view, view, phase, m, sec, partner).start()

    def scaled(buf, m, which, slot, gain):
        total = jnp.zeros((LEN, 128), F32)
        for j in range(CHIPS):
            block = which * CHIPS + j
            value = buf[m, block].astype(F32)
            total = total + value * value
            factor = gain[:, pl.ds(pl.multiple_of(block * 128, 128), 128)].astype(F32)
            xg[slot, :, j * 128 : (j + 1) * 128] = (value * factor).astype(BF)
        return total

    def inverse_rms(total):
        mean_sq = jnp.sum(total, axis=-1, keepdims=True) * (1.0 / D)
        return lax.rsqrt(mean_sq + EPSILON)

    def rows_of(which):
        return pl.ds(pl.multiple_of(which * (D // 2), D // 2), D // 2)

    def arrive(m):
        @pl.when(sec != 0)
        def _():
            received(yb.at[m], S_Y, m)
            gather_send(xa, S_AG1, m)

    def project(m):
        @pl.when(sec == 0)
        def _():
            received(xa.at[m, pl.ds(0, CHIPS)], S_IN, m)

        @pl.when(sec != 0)
        def _():
            received(xa.at[m, pl.ds(0, CHIPS - 1)], S_AG1, m)

        gather_pass(xa, S_PASS1, m)
        total = scaled(xa, m, core, 0, again)
        front, back = pl.ds(0, 2 * HD), pl.ds(2 * HD, HD)
        aq[:, front] = jnp.dot(xg[0], wqkv[rows_of(core), front], preferred_element_type=F32)

        @pl.when(sec != 0)
        def _():
            aq[:, back] = jnp.dot(xg[0], wqkv[rows_of(core), back], preferred_element_type=F32)

        received(xa.at[m, pl.ds(0, CHIPS)], S_PASS1, m)
        total = total + scaled(xa, m, rest, 1, again)
        scale = inverse_rms(total)
        qk = aq[:, front] + jnp.dot(xg[1], wqkv[rows_of(rest), front], preferred_element_type=F32)
        qk = qk * scale
        qs[m] = rotated(qk[:, :HD])

        @pl.when(sec != 0)
        def _():
            ks[m] = rotated(qk[:, HD:].astype(BF).astype(F32))
            v = aq[:, back] + jnp.dot(
                xg[1], wqkv[rows_of(rest), back], preferred_element_type=F32
            )
            vs[m] = (v * scale).astype(BF)

        @pl.when(sec == 0)
        def _():
            turned = qk[:, HD:].astype(BF).astype(F32).T
            pairs = jnp.concatenate([turned[0:32, :], turned[32:64, :]], axis=1)
            kvs[m] = pairs.reshape(KV_HEADS, 4, 128)
            kvr[m, me] = kvs[m, kv_id]

            def send(k, carry):
                d = lax.rem(me + k, N)
                remote(
                    kvs.at[m, d // (HEADS // KV_HEADS)], kvr.at[m, me], S_KV, m, sec, d
                ).start()
                return carry

            lax.fori_loop(1, N, send, 0)

    def rotated(value):
        mid = HD // 2
        swapped = jnp.concatenate([value[:, mid:], value[:, :mid]], axis=1)
        return (value * cs[...] + swapped * sn[...]).astype(BF)

    def reduce_send(left, weights, phase, pass_phase, recv, m):
        def term(which, i):
            first = which * (D // 2) + i * 1024
            cols = pl.ds(pl.multiple_of(first, 1024), 1024)
            return jnp.dot(left, weights[:, cols], preferred_element_type=F32)

        def away(i, carry):
            value = term(rest, i).astype(BF)
            for j in range(8):
                pt[phase - S_RS1, m, i * 8 + j] = value[:, j * 128 : (j + 1) * 128]
            return carry

        lax.fori_loop(0, 2, away, 0, unroll=True)
        give = remote(pt.at[phase - S_RS1, m], dr.at[phase - S_RS1, m], pass_phase, m, sec, partner)
        give.start()

        def kept(i, carry):
            value = term(core, i)
            for j in range(8):
                own[i * 8 + j] = value[:, j * 128 : (j + 1) * 128]
            return carry

        lax.fori_loop(0, 2, kept, 0, unroll=True)
        give.wait()

        def add(j, carry):
            ps[phase - S_RS1, m, j] = (own[j] + dr[phase - S_RS1, m, j].astype(F32)).astype(BF)
            return carry

        lax.fori_loop(0, CHIPS, add, 0, unroll=True)
        others(
            lambda chip_to: remote(
                ps.at[phase - S_RS1, m, chip_to], recv.at[m, chip], phase, m, sec,
                chip_to * 2 + core,
            ).start()
        )
        recv[m, chip] = ps[phase - S_RS1, m, chip]

    def summed(recv, phase, m):
        received(recv.at[m, pl.ds(0, CHIPS - 1)], phase, m)
        total = recv[m, 0].astype(F32)
        for j in range(1, CHIPS):
            total = total + recv[m, j].astype(F32)
        return total

    def attend(m):
        @pl.when(sec == 0)
        def _():
            received(kvr.at[m, pl.ds(0, N - 1)], S_KV, m)
            both = kvr[m].reshape(HD, 128).T
            ks[m] = rotated(both[:LEN])
            vs[m] = both[LEN:].astype(BF)

        scores = lax.dot_general(qs[m], ks[m], nt, preferred_element_type=F32) * HD ** (-0.5)
        row = lax.broadcasted_iota(jnp.int32, (LEN, LEN), 0)
        col = lax.broadcasted_iota(jnp.int32, (LEN, LEN), 1)
        scores = jnp.where(row >= col, scores, -jnp.inf)
        top = jnp.max(scores, axis=-1, keepdims=True)
        e = jnp.exp(scores - top)
        prob = (e / jnp.sum(e, axis=-1, keepdims=True)).astype(BF)
        context = jnp.dot(prob, vs[m], preferred_element_type=F32)
        on = jnp.full((LEN, HD), heads[m, 0], jnp.int32) > me
        context = jnp.where(on, context, 0.0).astype(BF)
        reduce_send(context, wob, S_RS1, S_GIVE1, r1, m)

    def attended(m):
        value = xa[m, mine].astype(F32) + summed(r1, S_RS1, m)
        att[m] = value
        xb[m, mine] = value.astype(BF)
        gather_send(xb, S_AG2, m)

    def feed(m):
        received(xb.at[m, pl.ds(0, CHIPS - 1)], S_AG2, m)
        gather_pass(xb, S_PASS2, m)
        total = scaled(xb, m, core, 0, fgain)

        def first(i, carry):
            cols = pl.ds(pl.multiple_of(i * 256, 256), 256)
            acc[0, :, cols] = jnp.dot(
                xg[0], wgb[rows_of(core), cols], preferred_element_type=F32
            )
            acc[1, :, cols] = jnp.dot(
                xg[0], wub[rows_of(core), cols], preferred_element_type=F32
            )
            return carry

        lax.fori_loop(0, 2, first, 0, unroll=True)
        received(xb.at[m, pl.ds(0, CHIPS)], S_PASS2, m)
        scale = inverse_rms(total + scaled(xb, m, rest, 1, fgain))
        limit = jnp.full((LEN, 256), blocks[m, 0], jnp.int32) * BLOCK

        def second(i, carry):
            cols = pl.ds(pl.multiple_of(i * 256, 256), 256)
            gate = acc[0, :, cols] + jnp.dot(
                xg[1], wgb[rows_of(rest), cols], preferred_element_type=F32
            )
            up = acc[1, :, cols] + jnp.dot(
                xg[1], wub[rows_of(rest), cols], preferred_element_type=F32
            )
            gate, up = gate * scale, up * scale
            ids = me * UNITS + i * 256 + lax.broadcasted_iota(jnp.int32, (LEN, 256), 1)
            value = gate / (1.0 + jnp.exp(-gate)) * up
            hbuf[:, cols] = jnp.where(ids < limit, value, 0.0).astype(BF)
            return carry

        lax.fori_loop(0, 2, second, 0, unroll=True)
        reduce_send(hbuf[...], wdb, S_RS2, S_GIVE2, r2, m)

    def finish(m):
        yb[m] = (att[m] + summed(r2, S_RS2, m)).astype(BF)

        @pl.when(sec < SECTIONS - 1)
        def _():
            remote(yb.at[m], xa.at[m, mine], S_Y, m, sec + 1, me).start()

        @pl.when((sec == SECTIONS - 1) & (m < MICRO - 1))
        def _():
            pltpu.make_async_remote_copy(
                src_ref=yb.at[m], dst_ref=obuf.at[0, mine], send_sem=send_sem.at[S_Y, m],
                recv_sem=misc_sem.at[2], device_id=(m, me), device_id_type=MESH,
            ).start()

    work = (arrive, project, attend, attended, feed, finish)
    waits = {2: weight[3:4], 4: weight[4:]}

    def step(t, carry):
        word = jnp.int32(0)
        for s in range(SECTIONS):
            for k in range(STEPS // PACK):
                here = (sec == s) & (t // PACK == k)
                word = jnp.where(here, jnp.int32(WORDS[s][k]), word)
        for k in range(PACK - 1):
            word = jnp.where(lax.rem(t, PACK) > k, word // 32, word)
        code = lax.rem(word, 32)
        kind, m = code // MICRO, lax.rem(code, MICRO)
        for i, fn in enumerate(work):
            @pl.when(kind == i)
            def _():
                if i in waits:
                    @pl.when(m == 0)
                    def _():
                        for w in waits[i]:
                            w.wait()

                fn(m)

        return carry

    lax.fori_loop(0, STEPS, step, 0)

    @pl.when(sec == SECTIONS - 1)
    def _():
        obuf[0, mine] = yb[MICRO - 1]

    @pl.when(sec != SECTIONS - 1)
    def _():
        pltpu.make_async_copy(yb.at[0], yb.at[0], misc_sem.at[2]).wait()

    gather_send(obuf, S_AG3, 0)
    received(obuf.at[0, pl.ds(0, CHIPS - 1)], S_AG3, 0)
    gather_pass(obuf, S_PASS3, 0)
    near = pltpu.make_async_copy(
        obuf.at[0, half(core)], out.at[half(core)], misc_sem.at[3]
    )
    near.start()

    def drain(m, carry):
        @pl.when(sec != 0)
        def _():
            sent(xa.at[m, pl.ds(0, CHIPS - 1)], S_AG1, m)

        sent(xa.at[m, pl.ds(0, CHIPS)], S_PASS1, m)

        @pl.when(sec == 0)
        def _():
            sent(kvr.at[m, pl.ds(0, N - 1)], S_KV, m)

        sent(r1.at[m, pl.ds(0, CHIPS - 1)], S_RS1, m)
        sent(xb.at[m, pl.ds(0, CHIPS - 1)], S_AG2, m)
        sent(xb.at[m, pl.ds(0, CHIPS)], S_PASS2, m)
        sent(r2.at[m, pl.ds(0, CHIPS - 1)], S_RS2, m)

        @pl.when((sec < SECTIONS - 1) | (m < MICRO - 1))
        def _():
            sent(yb.at[m], S_Y, m)

        return carry

    lax.fori_loop(0, MICRO, drain, 0)

    @pl.when(sec != 0)
    def _():
        pltpu.make_async_copy(x0, x0, misc_sem.at[1]).wait()

    sent(obuf.at[0, pl.ds(0, CHIPS - 1)], S_AG3, 0)
    received(obuf.at[0, pl.ds(0, CHIPS)], S_PASS3, 0)
    far = pltpu.make_async_copy(obuf.at[0, half(rest)], out.at[half(rest)], misc_sem.at[4])
    far.start()
    sent(obuf.at[0, pl.ds(0, CHIPS)], S_PASS3, 0)
    near.wait()
    far.wait()


def tables():
    half = HD // 2
    frequency = ROPE_BASE ** (-(np.arange(half, dtype=np.float64) / half))
    angles = np.arange(LEN, dtype=np.float64)[:, None] * frequency[None, :]
    c, s = np.cos(angles).astype(np.float32), np.sin(angles).astype(np.float32)
    cs = np.concatenate([c, c], axis=1)
    sn = np.concatenate([-s, s], axis=1)
    pk = np.zeros((32, HD), np.float32)
    pv = np.zeros((32, HD), np.float32)
    tk = np.zeros((64, 32), np.float32)
    tv = np.zeros((64, 32), np.float32)
    for j in range(4):
        for k in range(KV_HEADS):
            pk[j * KV_HEADS + k, k * 4 + j] = 1.0
            pv[j * KV_HEADS + k, 32 + k * 4 + j] = 1.0
            tk[k * 8 + j, j * KV_HEADS + k] = 1.0
            tv[k * 8 + 4 + j, j * KV_HEADS + k] = 1.0
    order = np.zeros((2 * HD, 2 * HD), np.float32)
    for c in range(2):
        for q in range(CHIPS):
            for r in range(4):
                row, col = (c * CHIPS + q) * 8 + r, 4 * (2 * q + c) + r
                order[row, col] = 1.0
                order[row + 4, HD + col] = 1.0
    return (jnp.asarray(cs), jnp.asarray(sn)) + tuple(
        jnp.asarray(a, BF) for a in (pk, pv, tk, tv, order)
    )


def per_device(*args):
    any_spec = pl.BlockSpec(memory_space=pl.ANY)
    vmem = pl.BlockSpec(memory_space=pltpu.VMEM)
    smem = pl.BlockSpec(memory_space=pltpu.SMEM)
    piece = (LEN, 128)
    gathered = pl.pallas_call(
        body,
        out_shape=jax.ShapeDtypeStruct((N, *piece), BF),
        in_specs=[
            any_spec, vmem, any_spec, any_spec, any_spec, any_spec, vmem, any_spec, any_spec,
            any_spec, smem, smem, vmem, vmem, vmem, vmem, vmem, vmem, vmem,
        ],
        out_specs=any_spec,
        scratch_shapes=[
            pltpu.VMEM((CHIPS, *piece), BF),
            pltpu.VMEM((MICRO, N, *piece), BF),
            pltpu.VMEM((MICRO, N, *piece), BF),
            pltpu.VMEM((MICRO, CHIPS, *piece), BF),
            pltpu.VMEM((MICRO, CHIPS, *piece), BF),
            pltpu.VMEM((2, MICRO, CHIPS, *piece), BF),
            pltpu.VMEM((2, MICRO, CHIPS, *piece), BF),
            pltpu.VMEM((2, MICRO, CHIPS, *piece), BF),
            pltpu.VMEM((CHIPS, *piece), F32),
            pltpu.VMEM((MICRO, KV_HEADS, 4, 128), F32),
            pltpu.VMEM((MICRO, N, 4, 128), F32),
            pltpu.VMEM((1, N, *piece), BF),
            pltpu.VMEM((MICRO, *piece), BF),
            pltpu.VMEM((MICRO, *piece), F32),
            pltpu.VMEM((2, LEN, D // 2), BF),
            pltpu.VMEM((2, LEN, UNITS), F32),
            pltpu.VMEM((LEN, UNITS), BF),
            pltpu.VMEM((MICRO, *piece), BF),
            pltpu.VMEM((MICRO, *piece), BF),
            pltpu.VMEM((MICRO, *piece), BF),
            pltpu.VMEM((LEN, 3 * HD), F32),
            pltpu.VMEM((KV_HEADS, 8, D), BF),
            pltpu.VMEM((N, 8, D), BF),
            pltpu.VMEM((D, 3 * HD), BF),
            pltpu.VMEM((D, 32), BF),
            pltpu.VMEM((D, 32), BF),
            pltpu.VMEM((HD, D), BF),
            pltpu.VMEM((D, UNITS), BF),
            pltpu.VMEM((D, UNITS), BF),
            pltpu.VMEM((UNITS, D), BF),
            pltpu.SemaphoreType.DMA((14, MICRO)),
            pltpu.SemaphoreType.DMA((14, MICRO)),
            pltpu.SemaphoreType.DMA((5,)),
            pltpu.SemaphoreType.DMA((7,)),
        ],
        compiler_params=pltpu.CompilerParams(
            collective_id=0, has_side_effects=True, vmem_limit_bytes=56 * 1024 * 1024
        ),
    )(*args, *tables())
    return gathered.transpose(1, 0, 2).reshape(1, 1, LEN, D)


def solution(mesh):
    return jax.shard_map(
        per_device,
        mesh=mesh,
        in_specs=(
            P(None, "section", None, None),
            P("section", None),
            P("section", None, "mp"),
            P("section", None, "mp"),
            P("section", None, "mp"),
            P("section", "mp", None),
            P("section", None),
            P("section", None, "mp"),
            P("section", None, "mp"),
            P("section", "mp", None),
            P(None, "section"),
            P(None, "section"),
        ),
        out_specs=P(None, "section", None, None),
        check_vma=False,
    )
```
